32 devices in a mesh: vehicle: 4 (over y, x), track: 2 (over core), cross: 4 (over z).
Axes of the slice: x: 2, y: 2, z: 4, core: 2. Of those that a mesh axis runs over, the one named last changes fastest.
Arguments:
- particle_offset: float32 [3, 16, 32, 128], P(None, ('vehicle', 'track'), 'cross'), may hold values from 0 to 1
- particle_velocity: float32 [3, 16, 32, 128], P(None, ('vehicle', 'track'), 'cross'), may hold values from -4 to 4
- cell_count: int32 [16, 32], P(('vehicle', 'track'), 'cross'), may hold values from 32 to 128
- face_offset: float32 [2048, 3, 128], P(('vehicle', 'track', 'cross')), may hold values from 0 to 1
- face_velocity: float32 [2048, 3, 128], P(('vehicle', 'track', 'cross')), may hold values from -4 to 4
- face_route: int32 [2048, 1], P(('vehicle', 'track', 'cross')), may hold values from 0 to 7; in each aligned block of 64 rows (0 to 63, 64 to 127, ...) at most 32 rows name the same one
- face_cell: int32 [2048], P(('vehicle', 'track', 'cross')), may hold values from 0 to 15
Outputs:
- moved_offset: float32 [3, 16, 32, 128], P(None, ('vehicle', 'track'), 'cross')
- new_velocity: float32 [3, 16, 32, 128], P(None, ('vehicle', 'track'), 'cross')
- face_impulse: float32 [2048, 3, 128], P(('vehicle', 'track', 'cross'))
The draws below stay inside these ranges and needn't reach their ends.
Inputs may be any that keep to these rules, and one draw needn't show every extreme that they name: `face_route`: among the 64 face blocks of one owner device, at most 32 name the same terrain device, and that many is reached.
All inputs are finite; a program needn't handle non-finite values.
Results may differ from the reference program's by a relative error of at most 0.0003.
Values sent between devices are 32-bit elements; how exact they have to be, the bound alone decides.
No kernel may reach another device: no remote copies, remote signals or barrier semaphores. Data moves between devices by JAX's collectives and lax.ppermute only.
A program may use at most 64 MiB of HBM per device.

```python
import math
import jax
import jax.numpy as jnp
import numpy as np
from jax import lax

CT = 2
CC = 8
SLOTS = 128
FACES = 128
FB_DEV = 64
CAP = 32
ROWS_T = 16
ROWS_C = 32
FBLOCKS = 2048
N_TRACK = 2
N_CROSS = 4


def set_ends(drawn, key, low, high):
    index_at = [jax.random.randint(jax.random.fold_in(key, axis), (), 0, length) for axis, length in enumerate(drawn.shape)]
    main_axis = drawn.shape.index(max(drawn.shape))
    beside = index_at[:main_axis] + [(index_at[main_axis] + 1) % drawn.shape[main_axis]] + index_at[main_axis + 1:]
    return drawn.at[tuple(index_at)].set(low).at[tuple(beside)].set(high)


def level_of(rng, shape, cuts, low, high):
    def one(dim, parts):
        heights = jax.random.uniform(jax.random.fold_in(jax.random.fold_in(rng, 6), dim), (parts,), jnp.float32, low / len(cuts), high / len(cuts))
        return jnp.repeat(jnp.exp(heights), shape[dim] // parts).reshape((-1,) + (1,) * (len(shape) - dim - 1))

    level = one(*cuts[0])
    for cut in cuts[1:]:
        level = level * one(*cut)
    return level


def routed_block(own_key, own, number, rows, number_of, top, bound, slope):
    sequence = jax.random.permutation(own_key, number_of)
    heavy_load, common = shares(number_of, rows * top, bound, slope, True), shares(number_of, rows * top, bound, slope, False)
    places = jnp.arange(number_of)

    def named(lengths, turn):
        used = int((lengths > 0).sum())
        fixed = max(1, used // 4)
        passed = fixed + (places - fixed + turn * (used - fixed)) % max(1, number_of - fixed)
        return jnp.zeros((number_of,), jnp.int32).at[sequence[jnp.where(places < fixed, places, passed)]].set(jnp.asarray(lengths, jnp.int32))

    lengths = jnp.where(number % 4 == 0, named(heavy_load, number // 4), named(common, number - number // 4 - 1))
    mixed = jax.random.permutation(jax.random.fold_in(own, 3), number_of)
    source_of, receiver = mixed[0:number_of // 2 * 2:2], mixed[1:number_of // 2 * 2:2]
    slack = jnp.minimum(lengths[source_of] - 1, bound - lengths[receiver]) // 2
    slack = jnp.where((source_of == sequence[0]) | (receiver == sequence[0]) | (lengths[receiver] == 0), 0, jnp.maximum(slack, 0))
    passed = jax.random.randint(jax.random.fold_in(own, 4), (number_of // 2,), 0, 1 << 20) % (slack + 1)
    lengths = lengths.at[source_of].add(-passed).at[receiver].add(passed)
    labels = jnp.searchsorted(jnp.cumsum(lengths), jnp.arange(rows * top), side="right").astype(jnp.int32)
    listing = labels.reshape(top, rows).T
    listing = listing[jax.random.permutation(jax.random.fold_in(own, 1), rows)]
    turn = jax.random.randint(jax.random.fold_in(own, 2), (rows, 1), 0, top)
    return jnp.take_along_axis(listing, (jnp.arange(top)[None, :] + turn) % top, axis=1)


def shares(amount, total, bound, skew, full):
    portions = [(1 << 20) // math.isqrt(rank ** skew) + 1 for rank in range(1, amount + 1)]
    largest = bound if full else min(bound, max(-(-total // amount), total * portions[0] // sum(portions)))
    least = 1 if total - largest >= amount - 1 else 0
    holding, surplus = [largest] + [least] * (amount - 1), total - largest - least * (amount - 1)
    while surplus > 0:
        free = [i for i in range(1, amount) if holding[i] < largest] or [i for i in range(1, amount) if holding[i] < bound]
        pool, remaining = sum([portions[i] for i in free]), surplus
        for i in free:
            addition = min(bound - holding[i], max(1, remaining * portions[i] // pool), surplus)
            holding[i] = holding[i] + addition
            surplus = surplus - addition
    return np.array(holding)


def centred(rng, dims, scale, most, cuts=(), held_as=jnp.bfloat16):
    entries = scale * jax.random.normal(rng, dims, jnp.float32)
    if cuts:
        entries = entries * level_of(rng, dims, cuts, -0.22, 0.18)
    return jnp.clip(entries, -most, most).astype(held_as)


def setup_inputs(seed: int = 0) -> dict:
    splits = jax.random.split(jax.random.key(seed), 8)
    particle_offset = jnp.clip(1.0 * jax.random.uniform(splits[0], (3, ROWS_T, ROWS_C, SLOTS), jnp.float32) ** level_of(splits[0], (3, ROWS_T, ROWS_C, SLOTS), ((1, 8), (2, 4)), -0.2, 0.2), 0.0, 1.0)
    particle_velocity = centred(splits[1], (3, ROWS_T, ROWS_C, SLOTS), 1.0, 4.0, ((1, 8), (2, 4)), jnp.float32)
    cell_count = set_ends(jax.random.randint(splits[2], (ROWS_T, ROWS_C), SLOTS // 4, SLOTS + 1), jax.random.fold_in(splits[2], 1), SLOTS // 4, SLOTS).astype(jnp.int32)
    face_offset = jnp.clip(1.0 * jax.random.uniform(splits[3], (FBLOCKS, 3, FACES), jnp.float32) ** level_of(splits[3], (FBLOCKS, 3, FACES), ((0, 32),), -0.2, 0.2), 0.0, 1.0)
    face_velocity = centred(splits[4], (FBLOCKS, 3, FACES), 1.0, 4.0, ((0, 32),), jnp.float32)
    face_route_keys = jax.random.split(jax.random.fold_in(splits[5], 1), FBLOCKS // FB_DEV)
    face_route_turns = jax.random.permutation(jax.random.fold_in(splits[5], 3), FBLOCKS // FB_DEV)
    face_route = jax.vmap(lambda own, number: routed_block(jax.random.fold_in(splits[5], 2), own, number, FB_DEV, N_TRACK * N_CROSS, 1, CAP, 2))(face_route_keys, face_route_turns).reshape((FBLOCKS, 1))
    face_cell = set_ends(jax.random.randint(splits[6], (FBLOCKS,), 0, CT * CC), jax.random.fold_in(splits[6], 1), 0, (CT * CC) - 1).astype(jnp.int32)
    return {"particle_offset": particle_offset, "particle_velocity": particle_velocity, "cell_count": cell_count, "face_offset": face_offset, "face_velocity": face_velocity, "face_route": face_route, "face_cell": face_cell}


radius = 0.1
face_radius = 0.15
stiffness = 100.0
damping = 40.0
soften = 0.05
time_step = 0.02
gravity = 9.81

def contact(own_pos, own_vel, other_pos, other_vel, other_live, reach):
    apart = own_pos[:, :, :, None] - other_pos[:, :, None, :]
    distance = jnp.sqrt(lax.optimization_barrier(jnp.sum(apart * apart, axis=0)) + soften * soften)
    normal = apart / distance[None]
    closing = lax.optimization_barrier(jnp.sum((own_vel[:, :, :, None] - other_vel[:, :, None, :]) * normal, axis=0))
    intersection = jnp.maximum(reach - distance, 0.0)
    weight = intersection * (stiffness - damping * closing) * other_live[:, None, :]
    return weight[None] * normal

def particle_forces(stacked, padded):
    across = stacked.shape[2]
    slot_count = stacked.shape[3]
    others = 1.0 - jnp.eye(slot_count, dtype=jnp.float32)

    def row_force(row_index):
        own_part = lax.dynamic_slice_in_dim(stacked, row_index, 1, 1)[:, 0]
        total_force = jnp.zeros((3, across, slot_count), jnp.float32)
        for shift_t in (-1, 0, 1):
            band_rows = lax.dynamic_slice_in_dim(padded, row_index + 1 + shift_t, 1, 1)[:, 0]
            for shift_c in (-1, 0, 1):
                neighbour = band_rows[:, 1 + shift_c:1 + shift_c + across]
                offset = jnp.array([shift_t, shift_c, 0.0], jnp.float32)[:, None, None]
                pushes = contact(own_part[0:3], own_part[3:6], neighbour[0:3] + offset, neighbour[3:6], neighbour[6], 2.0 * radius)
                if shift_t == 0 and shift_c == 0:
                    pushes = pushes * others
                total_force = total_force + lax.optimization_barrier(jnp.sum(pushes, axis=3))
        return total_force * own_part[6][None]
    forces = lax.map(row_force, jnp.arange(stacked.shape[1], dtype=jnp.int32))
    return jnp.transpose(forces, (1, 0, 2, 3))

def tire_contact(chosen, face_pos, face_vel):
    ones_live = jnp.ones((face_pos.shape[1], face_pos.shape[2]), jnp.float32)
    pushes = contact(chosen[0:3], chosen[3:6], face_pos, face_vel, ones_live, radius + face_radius)
    pushes = pushes * chosen[6][None, :, :, None]
    return (lax.optimization_barrier(jnp.sum(pushes, axis=3)), -lax.optimization_barrier(jnp.sum(pushes, axis=2)))

def reference(particle_offset, particle_velocity, cell_count, face_offset, face_velocity, face_route, face_cell):
    travel_rows, cross_rows, slot_count = particle_offset.shape[1:]
    faces = face_offset.shape[2]
    live = (lax.broadcasted_iota(jnp.int32, (travel_rows, cross_rows, slot_count), 2) < cell_count[:, :, None]).astype(jnp.float32)
    owners = jnp.arange(FBLOCKS, dtype=jnp.int32) // FB_DEV
    vehicle_index = owners // (N_TRACK * N_CROSS)
    target = face_route[:, 0]
    block_t = (vehicle_index * N_TRACK + target // N_CROSS) * CT + face_cell // CC
    block_c = target % N_CROSS * CC + face_cell % CC
    fall = jnp.array([0.0, 0.0, -gravity], jnp.float32)[:, None, None, None]
    groups = FBLOCKS // FB_DEV
    offsets = particle_offset
    velocity = particle_velocity
    reaction = jnp.zeros((FBLOCKS, 3, faces), jnp.float32)
    vel_spans = jnp.transpose(face_velocity.reshape(groups, FB_DEV, 3, faces), (0, 2, 1, 3))
    for substep in range(2):
        stacked = jnp.concatenate([offsets, velocity, live[None]], axis=0)
        padded = jnp.pad(stacked, ((0, 0), (1, 1), (1, 1), (0, 0)))
        total_push = particle_forces(stacked, padded)
        chosen = stacked[:, block_t, block_c, :]
        chosen_spans = jnp.transpose(chosen.reshape(7, groups, FB_DEV, slot_count), (1, 0, 2, 3))
        faces_now = face_offset + substep * time_step * face_velocity
        pos_spans = jnp.transpose(faces_now.reshape(groups, FB_DEV, 3, faces), (0, 2, 1, 3))

        def face_group(pieces):
            return tire_contact(pieces[0], pieces[1], pieces[2])
        on_particles, on_faces = lax.map(face_group, (chosen_spans, pos_spans, vel_spans))
        on_particles = jnp.transpose(on_particles, (1, 0, 2, 3)).reshape(3, FBLOCKS, slot_count)
        on_faces = jnp.transpose(on_faces, (0, 2, 1, 3)).reshape(FBLOCKS, 3, faces)
        total_push = total_push.at[:, block_t, block_c, :].add(on_particles)
        velocity = velocity + time_step * (total_push + fall)
        offsets = offsets + time_step * velocity
        reaction = reaction + on_faces
    return (offsets, velocity, time_step * reaction)
```

```python
import functools

import jax
import jax.numpy as jnp
from jax import lax
from jax.experimental import pallas as pl
from jax.experimental.pallas import tpu as pltpu
from jax.sharding import PartitionSpec as P

radius = 0.1
face_radius = 0.15
stiffness = 100.0
damping = 40.0
soften = 0.05
time_step = 0.02
gravity = 9.81

far = 1000.0
f32 = jnp.float32
bf16 = jnp.bfloat16
falls = (0.0, 0.0, -gravity)
VMEM = pltpu.VMEM
SMEM = pltpu.SMEM


def split3(a):
    high = a.astype(bf16).astype(f32)
    rest = a - high
    mid = rest.astype(bf16).astype(f32)
    return high, mid, rest - mid


def features(state, eps):
    row = lax.broadcasted_iota(jnp.int32, state.shape, 0)
    turned = pltpu.roll(state, 5, 0)
    square = jnp.sum(jnp.where(row < 3, state * state, 0.0), axis=0, keepdims=True) + eps
    cross = jnp.sum(jnp.where(row < 3, state * turned, 0.0), axis=0, keepdims=True)
    full = jnp.where(row == 6, square, jnp.where(row == 7, cross, state))
    return split3(full), row


def left_side(pieces, row):
    p1, p2, p3 = pieces
    ones = jnp.where(row >= 6, 1.0, 0.0)
    zero = jnp.zeros_like(p1)
    stack = jnp.concatenate([p1, p1, p2, p1, p3, p2, ones, ones, ones, zero], axis=0)
    return jnp.transpose(stack).astype(bf16)


def right_side(pieces, row):
    def for_square(p, first):
        return jnp.where(row < 3, -2.0 * p, jnp.where(row == 6, 1.0 if first else 0.0, 0.0))

    def for_closing(p, first):
        swapped = jnp.where(row < 3, pltpu.roll(p, 5, 0), pltpu.roll(p, 3, 0))
        return jnp.where(row < 6, -swapped, jnp.where(row == 7, 1.0 if first else 0.0, 0.0))

    halves = []
    for side, keep in ((for_square, 6), (for_closing, 7)):
        b1, b2, b3 = [side(p, k == 0) for k, p in enumerate(pieces)]
        q = [jnp.where(row == keep, p, 0.0) for p in pieces]
        halves.append(jnp.concatenate([b1, b2, b1, b3, b1, b2] + q + [jnp.zeros_like(b1)], axis=0))
    return jnp.concatenate(halves, axis=1).astype(bf16)


def sum_side(pieces):
    p1, p2, p3 = pieces
    stack = jnp.concatenate([p1, p2, p3, jnp.ones_like(p1)], axis=0).astype(bf16)
    return jnp.concatenate([stack, stack], axis=1)


def pair_weights(product, reach):
    n = product.shape[1] // 2
    square = jnp.maximum(product[:, :n], soften * soften * 0.5)
    inverse = lax.rsqrt(square)
    weight = jnp.maximum(reach * inverse - 1.0, 0.0) * (
        stiffness / damping - product[:, n:] * inverse
    )
    high = weight.astype(bf16)
    low = (weight - high.astype(f32)).astype(bf16)
    return high, low


def dot(a, b, contract=((1,), (0,))):
    return lax.dot_general(a, b, (contract, ((), ())), preferred_element_type=f32)


def moment(state, sums):
    total = sums[0:8] + sums[8:16] + sums[16:24]
    return state * sums[24:25] - total


def advanced(x, v, force, axis):
    v = v + time_step * (force + falls[axis])
    return x + time_step * v, v


def put_own(state_ref, x_ref, v_ref, ct, cc):
    cells = lax.broadcasted_iota(jnp.int32, (cc, 128), 0).astype(f32)
    for r in range(ct):
        base = ((r + 1) * (cc + 2) + 1) * 8
        for axis in range(3):
            x = x_ref[axis, pl.ds(r * cc, cc), :]
            if axis == 0:
                x = x + (r + 1 - (ct + 1) / 2)
            if axis == 1:
                x = x + (cells + (1 - (cc + 1) / 2))
            state_ref[pl.ds(base + axis, cc, stride=8), :] = x
            state_ref[pl.ds(base + 3 + axis, cc, stride=8), :] = v_ref[axis, pl.ds(r * cc, cc), :]


def put_dead(state_ref, slot):
    row = lax.broadcasted_iota(jnp.int32, (8, 128), 0)
    state_ref[pl.ds(slot * 8, 8), :] = jnp.where(row == 0, far, 0.0)


def build_left(state_ref, left_ref, sum_ref, slots):
    for slot in slots:
        pieces, row = features(state_ref[pl.ds(slot * 8, 8), :], 0.0)
        left_ref[slot] = left_side(pieces, row)
        sum_ref[slot] = sum_side(pieces)


def build_right(state_ref, right_ref, slots):
    for k, slot in enumerate(slots):
        pieces, row = features(state_ref[pl.ds(slot * 8, 8), :], soften * soften)
        right_ref[k] = right_side(pieces, row)


def pushes(left_ref, sum_ref, right, others):
    total = None
    for slot in others:
        high, low = pair_weights(dot(left_ref[slot], right), 2.0 * radius)
        part = dot(sum_ref[slot], jnp.concatenate([high, low], axis=0))
        total = part if total is None else total + part
    return total


def store_rows(out_ref, values, index, add):
    for axis in range(3):
        line = damping * values[axis : axis + 1]
        if add:
            line = line + out_ref[axis, pl.ds(index, 1), :]
        out_ref[axis, pl.ds(index, 1), :] = line


def inner_kernel(ct, cc, x_ref, v_ref, out_ref, state_ref, left_ref, sum_ref, right_ref):
    wide = cc + 2
    own = [(r + 1) * wide + c + 1 for r in range(ct) for c in range(cc)]
    ends = [(r + 1) * wide + c for r in range(ct) for c in (0, cc + 1)]
    put_own(state_ref, x_ref, v_ref, ct, cc)
    for slot in ends:
        put_dead(state_ref, slot)
    build_left(state_ref, left_ref, sum_ref, own + ends)
    build_right(state_ref, right_ref, own)

    def column(c, carry):
        for r in range(ct):
            others = [
                (q + 1) * wide + c + d
                for q in range(max(r - 1, 0), min(r + 2, ct))
                for d in range(3)
            ]
            sums = pushes(left_ref, sum_ref, right_ref[r * cc + c], others)
            state = state_ref[pl.ds(pl.multiple_of(((r + 1) * wide + c + 1) * 8, 8), 8), :]
            store_rows(out_ref, moment(state, sums), r * cc + c, False)
        return carry

    lax.fori_loop(0, cc, column, 0)


def outer_kernel(ct, cc, crosses, second, s_ref, x_ref, v_ref, all_ref, halo_ref, *rest):
    if second:
        force_ref, halo_force_ref, *rest = rest
    out_ref, state_ref, left_ref, sum_ref, right_ref = rest
    wide = cc + 2
    c_index = s_ref[0]
    own_track = s_ref[1]
    has_low = c_index > 0
    has_high = c_index < crosses - 1
    put_own(state_ref, x_ref, v_ref, ct, cc)

    def place(slot, rr, p, load, ok):
        for axis in range(3):
            x, v = load(axis, 6, 0), load(axis + 3, 6, 0)
            if second:
                x, v = advanced(x, v, load(axis, 3, 1), axis)
            if axis == 0:
                x = x + (rr - (ct + 1) / 2)
                x = jnp.where(ok, x, far)
            if axis == 1:
                x = jnp.where(ok, x + (p - (cc + 1) / 2), 0.0)
            state_ref[pl.ds(slot * 8 + axis, 1), :] = x
            state_ref[pl.ds(slot * 8 + 3 + axis, 1), :] = jnp.where(ok, v, 0.0)

    def from_all(track, row, p):
        shift = -1 if p == 0 else (1 if p == cc + 1 else 0)
        device = track * crosses + jnp.clip(c_index + shift, 0, crosses - 1)
        cell = row * cc + (p - 1) % cc
        refs = (all_ref, force_ref) if second else (all_ref,)
        return lambda f, n, k: refs[k][device, f, pl.ds(cell, 1), :]

    def from_halo(p):
        refs = (halo_ref, halo_force_ref) if second else (halo_ref,)
        return lambda f, n, k: refs[k][pl.ds(p * n + f, 1), :]

    for rr, row, at in ((0, ct - 1, 2), (ct + 1, 0, 5)):
        inside, track, exists = s_ref[at] > 0, s_ref[at + 1], s_ref[at + 2] > 0
        for p in range(wide):
            a, b = from_all(track, row, p), from_halo(p)

            def load(f, n, k, a=a, b=b):
                return jnp.where(inside, a(f, n, k), b(f, n, k))

            ok = exists
            if p == 0:
                ok = jnp.logical_and(ok, has_low)
            if p == cc + 1:
                ok = jnp.logical_and(ok, has_high)
            place(rr * wide + p, rr, p, load, ok)
    for r in range(ct):
        place((r + 1) * wide, r + 1, 0, from_all(own_track, r, 0), has_low)
        place((r + 1) * wide + cc + 1, r + 1, cc + 1, from_all(own_track, r, cc + 1), has_high)
    ring = [rr * wide + p for rr in (0, ct + 1) for p in range(wide)]
    ring += [(r + 1) * wide + p for r in range(ct) for p in (0, cc + 1)]
    build_left(state_ref, left_ref, sum_ref, ring)
    build_right(state_ref, right_ref, [(r + 1) * wide + c + 1 for r in range(ct) for c in range(cc)])

    def one(r, c, others, add):
        sums = pushes(left_ref, sum_ref, right_ref[r * cc + c], others)
        start = ((r + 1) * wide + c + 1) * 8
        state = state_ref[pl.ds(start if add else pl.multiple_of(start, 8), 8), :]
        store_rows(out_ref, moment(state, sums), r * cc + c, add)

    if ct > 2:
        out_ref[...] = jnp.zeros_like(out_ref)

    def column(c, carry):
        one(0, c, [c + d for d in range(3)], False)
        one(ct - 1, c, [(ct + 1) * wide + c + d for d in range(3)], ct == 1)
        return carry

    lax.fori_loop(0, cc, column, 0)
    for r in range(ct):
        near = range(max(r - 1, 0), min(r + 2, ct))
        one(r, 0, [(q + 1) * wide for q in near], True)
        one(r, cc - 1, [(q + 1) * wide + cc + 1 for q in near], True)


def face_kernel(second, index_ref, offset_ref, velocity_ref, all_ref, *rest):
    if second:
        force_ref, *rest = rest
    part_ref, react_ref, state_ref, face_ref = rest
    devices, _, cells, _ = all_ref.shape
    count = offset_ref.shape[0]

    def spread(device, carry):
        base = pl.multiple_of(device * cells * 8, 8)
        for axis in range(3):
            x, v = all_ref[device, axis], all_ref[device, axis + 3]
            if second:
                x, v = advanced(x, v, force_ref[device, axis], axis)
            state_ref[pl.ds(base + axis, cells, stride=8), :] = x
            state_ref[pl.ds(base + 3 + axis, cells, stride=8), :] = v
            part_ref[device, axis] = jnp.zeros_like(x)
        return carry

    lax.fori_loop(0, devices, spread, 0)
    for axis in range(3):
        y, w = offset_ref[:, axis, :], velocity_ref[:, axis, :]
        if second:
            y = y + time_step * w
        face_ref[pl.ds(axis, count, stride=8), :] = y
        face_ref[pl.ds(3 + axis, count, stride=8), :] = w

    def one(f):
        block = index_ref[f]
        state = state_ref[pl.ds(pl.multiple_of(block * 8, 8), 8), :]
        face = face_ref[pl.ds(pl.multiple_of(f * 8, 8), 8), :]
        pieces, row = features(state, soften * soften)
        face_pieces, _ = features(face, 0.0)
        product = dot(left_side(face_pieces, row), right_side(pieces, row))
        high, low = pair_weights(product, radius + face_radius)
        onto = moment(state, dot(sum_side(face_pieces), jnp.concatenate([high, low], axis=0)))
        back = moment(
            face, dot(sum_side(pieces), jnp.concatenate([high, low], axis=1), ((1,), (1,)))
        )
        react_ref[f] = (time_step * damping * back)[0:3]
        return block, onto

    group = 4 if count % 4 == 0 else 1

    def several(g, carry):
        done = [one(g * group + k) for k in range(group)]
        for block, onto in done:
            device, cell = block // cells, block % cells
            for axis in range(3):
                line = part_ref[device, axis, pl.ds(cell, 1), :]
                part_ref[device, axis, pl.ds(cell, 1), :] = line + damping * onto[axis : axis + 1]
        return carry

    lax.fori_loop(0, count // group, several, 0)


def pack_kernel(cc, s_ref, mine_ref, out_ref):
    crosses, fields, _, _ = mine_ref.shape
    c_index, row = s_ref[0], s_ref[8]
    for p in range(cc + 2):
        shift = -1 if p == 0 else (1 if p == cc + 1 else 0)
        device = jnp.clip(c_index + shift, 0, crosses - 1)
        cell = row * cc + (p - 1) % cc
        for f in range(fields):
            out_ref[pl.ds(p * fields + f, 1), :] = mine_ref[device, f, pl.ds(cell, 1), :]


def call(kernel, name, args, scalars, outs, scratch, flops):
    specs = [pl.BlockSpec(memory_space=SMEM)] * scalars
    specs += [pl.BlockSpec(memory_space=VMEM)] * (len(args) - scalars)
    return pl.pallas_call(
        kernel,
        name=name,
        out_shape=[jax.ShapeDtypeStruct(s, f32) for s in outs],
        in_specs=specs,
        out_specs=[pl.BlockSpec(memory_space=VMEM)] * len(outs),
        scratch_shapes=scratch,
        cost_estimate=pl.CostEstimate(flops=flops, transcendentals=0, bytes_accessed=0),
    )(*args)


def body(
    particle_offset,
    particle_velocity,
    cell_count,
    face_offset,
    face_velocity,
    face_route,
    face_cell,
):
    _, ct, cc, slots = particle_offset.shape
    cells = ct * cc
    own_faces, _, faces = face_offset.shape
    vehicles, tracks, crosses = [lax.axis_size(a) for a in ("vehicle", "track", "cross")]
    vehicle, track, cross = [lax.axis_index(a) for a in ("vehicle", "track", "cross")]
    pair = tracks == 2
    wide = cc + 2
    grid_slots = (ct + 2) * wide
    ring_slots = [
        VMEM((grid_slots * 8, slots), f32),
        VMEM((grid_slots, slots, 80), bf16),
        VMEM((grid_slots, 32, 2 * slots), bf16),
        VMEM((cells, 80, 2 * slots), bf16),
    ]

    x = particle_offset.reshape(3, cells, slots)
    v = particle_velocity.reshape(3, cells, slots)
    live = (
        lax.broadcasted_iota(jnp.int32, (cells, slots), 1) < cell_count.reshape(cells)[:, None]
    )
    first = lax.broadcasted_iota(jnp.int32, (3, 1, 1), 0) == 0

    def marked(x):
        return jnp.where(first & ~live[None], far, x)

    def place(t):
        return jnp.bitwise_xor(t, track) if pair else t

    low, high = track > 0, track < tracks - 1
    target = face_route[:, 0]
    index = (place(target // crosses) * crosses + target % crosses) * cells + face_cell
    scalars = jnp.stack(
        [
            cross,
            place(track),
            low,
            place(jnp.maximum(track - 1, 0)),
            low | (vehicle > 0),
            high,
            place(jnp.minimum(track + 1, tracks - 1)),
            high | (vehicle < vehicles - 1),
            jnp.where(high, 0, ct - 1),
        ]
    ).astype(jnp.int32)
    swap = [(0, 1), (1, 0)]
    travel = []
    for e in range(vehicles - 1):
        last, following = e * tracks + tracks - 1, (e + 1) * tracks
        travel += [(last, following), (following, last)]

    def gather_cross(a):
        spread = jnp.broadcast_to(a[None], (crosses,) + a.shape)
        return lax.all_to_all(spread, "cross", split_axis=0, concat_axis=0, tiled=True)

    def gather_track(a):
        if pair:
            return jnp.concatenate([a, lax.ppermute(a, "track", swap)], axis=0)
        return lax.all_gather(a, "track", axis=0, tiled=True)

    def halo(a):
        packed = call(
            functools.partial(pack_kernel, cc),
            "pack",
            [scalars, a],
            1,
            [(wide * a.shape[1], slots)],
            [],
            1000,
        )[0]
        return lax.ppermute(packed, ("vehicle", "track"), travel)

    def scatter_force(part):
        part = part.reshape(tracks, crosses, 3, cells, slots)
        if pair:
            part = part[0] + lax.ppermute(part[1], "track", swap)
        else:
            part = jnp.sum(lax.all_to_all(part, "track", 0, 0, tiled=True), axis=0)
        return jnp.sum(lax.all_to_all(part, "cross", 0, 0, tiled=True), axis=0)

    fall = jnp.array(falls, f32)[:, None, None]
    reaction = None
    everyone = beyond = None
    force = None
    for substep in range(2):
        second = substep == 1
        own = marked(x)
        mine = gather_cross(force if second else jnp.concatenate([own, v], axis=0))
        inner = call(
            functools.partial(inner_kernel, ct, cc),
            "inner",
            [own, v],
            0,
            [(3, cells, slots)],
            ring_slots,
            4 * 10**9,
        )[0]
        group, across = gather_track(mine), halo(mine)
        if second:
            extra, halo_extra = [group], [across]
        else:
            everyone, beyond, extra, halo_extra = group, across, [], []
        part, react = call(
            functools.partial(face_kernel, second),
            "faces",
            [index, face_offset, face_velocity, everyone] + extra,
            1,
            [(tracks * crosses, 3, cells, slots), (own_faces, 3, faces)],
            [
                VMEM((tracks * crosses * cells * 8, slots), f32),
                VMEM((own_faces * 8, faces), f32),
            ],
            4 * 10**9,
        )
        outer = call(
            functools.partial(outer_kernel, ct, cc, crosses, second),
            "outer",
            [scalars, own, v, everyone, beyond] + extra + halo_extra,
            1,
            [(3, cells, slots)],
            ring_slots,
            4 * 10**9,
        )[0]
        force = jnp.where(live[None], inner + outer, 0.0) + scatter_force(part)
        v = v + time_step * (force + fall)
        x = x + time_step * v
        reaction = react if reaction is None else reaction + react
    shape = particle_offset.shape
    return (x.reshape(shape), v.reshape(shape), reaction)


def solution(mesh):
    in_specs = (
        P(None, ("vehicle", "track"), "cross", None),
        P(None, ("vehicle", "track"), "cross", None),
        P(("vehicle", "track"), "cross"),
        P(("vehicle", "track", "cross"), None, None),
        P(("vehicle", "track", "cross"), None, None),
        P(("vehicle", "track", "cross"), None),
        P(("vehicle", "track", "cross")),
    )
    out_specs = (
        P(None, ("vehicle", "track"), "cross", None),
        P(None, ("vehicle", "track"), "cross", None),
        P(("vehicle", "track", "cross"), None, None),
    )
    return jax.shard_map(body, mesh=mesh, in_specs=in_specs, out_specs=out_specs, check_vma=False)
```

```python
import functools

import jax
import jax.numpy as jnp
from jax import lax
from jax.experimental import pallas as pl
from jax.experimental.pallas import tpu as pltpu
from jax.sharding import PartitionSpec as P

radius = 0.1
face_radius = 0.15
stiffness = 100.0
damping = 40.0
soften = 0.05
time_step = 0.02
gravity = 9.81

far = 1000.0
ahead = 8
columns = 4
faces_at_once = 16
f32 = jnp.float32
bf16 = jnp.bfloat16
falls = (0.0, 0.0, -gravity)
VMEM = pltpu.VMEM
SMEM = pltpu.SMEM


def split3(a):
    high = a.astype(bf16).astype(f32)
    rest = a - high
    mid = rest.astype(bf16).astype(f32)
    return high, mid, rest - mid


def features(state, eps):
    row = lax.broadcasted_iota(jnp.int32, state.shape, 0)
    turned = pltpu.roll(state, 5, 0)
    square = jnp.sum(jnp.where(row < 3, state * state, 0.0), axis=0, keepdims=True) + eps
    cross = jnp.sum(jnp.where(row < 3, state * turned, 0.0), axis=0, keepdims=True)
    full = jnp.where(row == 6, square, jnp.where(row == 7, cross, state))
    return split3(full), row


def left_side(pieces, row):
    p1, p2, p3 = pieces
    ones = jnp.where(row >= 6, 1.0, 0.0)
    zero = jnp.zeros_like(p1)
    stack = jnp.concatenate([p1, p1, p2, p1, p3, p2, ones, ones, ones, zero], axis=0)
    return jnp.transpose(stack).astype(bf16)


def right_side(pieces, row):
    def for_square(p, first):
        return jnp.where(row < 3, -2.0 * p, jnp.where(row == 6, 1.0 if first else 0.0, 0.0))

    def for_closing(p, first):
        swapped = jnp.where(row < 3, pltpu.roll(p, 5, 0), pltpu.roll(p, 3, 0))
        return jnp.where(row < 6, -swapped, jnp.where(row == 7, 1.0 if first else 0.0, 0.0))

    halves = []
    for side, keep in ((for_square, 6), (for_closing, 7)):
        b1, b2, b3 = [side(p, k == 0) for k, p in enumerate(pieces)]
        q = [jnp.where(row == keep, p, 0.0) for p in pieces]
        halves.append(jnp.concatenate([b1, b2, b1, b3, b1, b2] + q + [jnp.zeros_like(b1)], axis=0))
    return jnp.concatenate(halves, axis=1).astype(bf16)


def sum_side(pieces):
    p1, p2, p3 = pieces
    stack = jnp.concatenate([p1, p2, p3, jnp.ones_like(p1)], axis=0).astype(bf16)
    return jnp.concatenate([stack, stack], axis=1)


def pair_weights(product, reach):
    n = product.shape[1] // 2
    square = jnp.maximum(product[:, :n], soften * soften * 0.5)
    inverse = lax.rsqrt(square)
    weight = jnp.maximum(reach * inverse - 1.0, 0.0) * (
        stiffness / damping - product[:, n:] * inverse
    )
    high = weight.astype(bf16)
    low = (weight - high.astype(f32)).astype(bf16)
    return high, low


def dot(a, b, contract=((1,), (0,))):
    return lax.dot_general(a, b, (contract, ((), ())), preferred_element_type=f32)


def moment(state, sums):
    total = sums[0:8] + sums[8:16] + sums[16:24]
    return state * sums[24:25] - total


def advanced(x, v, force, axis):
    v = v + time_step * (force + falls[axis])
    return x + time_step * v, v


def put_own(state_ref, x_ref, v_ref, ct, cc):
    cells = lax.broadcasted_iota(jnp.int32, (cc, 128), 0).astype(f32)
    for r in range(ct):
        base = ((r + 1) * (cc + 2) + 1) * 8
        for axis in range(3):
            x = x_ref[axis, pl.ds(r * cc, cc), :]
            if axis == 0:
                x = x + (r + 1 - (ct + 1) / 2)
            if axis == 1:
                x = x + (cells + (1 - (cc + 1) / 2))
            state_ref[pl.ds(base + axis, cc, stride=8), :] = x
            state_ref[pl.ds(base + 3 + axis, cc, stride=8), :] = v_ref[axis, pl.ds(r * cc, cc), :]


def put_dead(state_ref, slot):
    row = lax.broadcasted_iota(jnp.int32, (8, 128), 0)
    state_ref[pl.ds(slot * 8, 8), :] = jnp.where(row == 0, far, 0.0)


def build_left(state_ref, left_ref, sum_ref, slots):
    for slot in slots:
        pieces, row = features(state_ref[pl.ds(slot * 8, 8), :], 0.0)
        left_ref[slot] = left_side(pieces, row)
        sum_ref[slot] = sum_side(pieces)


def build_right(state_ref, right_ref, slots):
    for k, slot in enumerate(slots):
        pieces, row = features(state_ref[pl.ds(slot * 8, 8), :], soften * soften)
        right_ref[k] = right_side(pieces, row)


def pushes(left_ref, sum_ref, right_ref, jobs):
    todo = [(k, block, slot) for k, (block, others) in enumerate(jobs) for slot in others]
    totals = [None] * len(jobs)
    waiting = []
    for n in range(len(todo) + ahead):
        if n < len(todo):
            k, block, slot = todo[n]
            waiting.append((k, slot, dot(left_ref[slot], right_ref[block])))
        if n >= ahead:
            k, slot, product = waiting.pop(0)
            high, low = pair_weights(product, 2.0 * radius)
            part = dot(sum_ref[slot], jnp.concatenate([high, low], axis=0))
            totals[k] = part if totals[k] is None else totals[k] + part
    return totals


def store_rows(out_ref, values, index, add):
    for axis in range(3):
        line = damping * values[axis : axis + 1]
        if add:
            line = line + out_ref[axis, pl.ds(index, 1), :]
        out_ref[axis, pl.ds(index, 1), :] = line


def inner_kernel(ct, cc, x_ref, v_ref, out_ref, state_ref, left_ref, sum_ref, right_ref):
    wide = cc + 2
    own = [(r + 1) * wide + c + 1 for r in range(ct) for c in range(cc)]
    ends = [(r + 1) * wide + c for r in range(ct) for c in (0, cc + 1)]
    put_own(state_ref, x_ref, v_ref, ct, cc)
    for slot in ends:
        put_dead(state_ref, slot)
    build_left(state_ref, left_ref, sum_ref, own + ends)
    build_right(state_ref, right_ref, own)

    def several(step, carry):
        jobs, places = [], []
        for k in range(columns):
            c = step * columns + k
            for r in range(ct):
                near = range(max(r - 1, 0), min(r + 2, ct))
                jobs.append((r * cc + c, [(q + 1) * wide + c + d for q in near for d in range(3)]))
                places.append(((r + 1) * wide + c + 1, r * cc + c))
        for sums, (slot, index) in zip(pushes(left_ref, sum_ref, right_ref, jobs), places):
            state = state_ref[pl.ds(pl.multiple_of(slot * 8, 8), 8), :]
            store_rows(out_ref, moment(state, sums), index, False)
        return carry

    lax.fori_loop(0, cc // columns, several, 0)


def outer_kernel(ct, cc, crosses, second, s_ref, x_ref, v_ref, all_ref, halo_ref, *rest):
    if second:
        force_ref, halo_force_ref, *rest = rest
    out_ref, state_ref, left_ref, sum_ref, right_ref = rest
    wide = cc + 2
    c_index = s_ref[0]
    own_track = s_ref[1]
    has_low = c_index > 0
    has_high = c_index < crosses - 1
    put_own(state_ref, x_ref, v_ref, ct, cc)

    def place(slot, rr, p, load, ok):
        for axis in range(3):
            x, v = load(axis, 6, 0), load(axis + 3, 6, 0)
            if second:
                x, v = advanced(x, v, load(axis, 3, 1), axis)
            if axis == 0:
                x = x + (rr - (ct + 1) / 2)
                x = jnp.where(ok, x, far)
            if axis == 1:
                x = jnp.where(ok, x + (p - (cc + 1) / 2), 0.0)
            state_ref[pl.ds(slot * 8 + axis, 1), :] = x
            state_ref[pl.ds(slot * 8 + 3 + axis, 1), :] = jnp.where(ok, v, 0.0)

    def from_all(track, row, p):
        shift = -1 if p == 0 else (1 if p == cc + 1 else 0)
        device = track * crosses + jnp.clip(c_index + shift, 0, crosses - 1)
        cell = row * cc + (p - 1) % cc
        refs = (all_ref, force_ref) if second else (all_ref,)
        return lambda f, n, k: refs[k][device, f, pl.ds(cell, 1), :]

    def from_halo(p):
        refs = (halo_ref, halo_force_ref) if second else (halo_ref,)
        return lambda f, n, k: refs[k][pl.ds(p * n + f, 1), :]

    for rr, row, at in ((0, ct - 1, 2), (ct + 1, 0, 5)):
        inside, track, exists = s_ref[at] > 0, s_ref[at + 1], s_ref[at + 2] > 0
        for p in range(wide):
            a, b = from_all(track, row, p), from_halo(p)

            def load(f, n, k, a=a, b=b):
                return jnp.where(inside, a(f, n, k), b(f, n, k))

            ok = exists
            if p == 0:
                ok = jnp.logical_and(ok, has_low)
            if p == cc + 1:
                ok = jnp.logical_and(ok, has_high)
            place(rr * wide + p, rr, p, load, ok)
    for r in range(ct):
        place((r + 1) * wide, r + 1, 0, from_all(own_track, r, 0), has_low)
        place((r + 1) * wide + cc + 1, r + 1, cc + 1, from_all(own_track, r, cc + 1), has_high)
    ring = [rr * wide + p for rr in (0, ct + 1) for p in range(wide)]
    ring += [(r + 1) * wide + p for r in range(ct) for p in (0, cc + 1)]
    build_left(state_ref, left_ref, sum_ref, ring)
    build_right(state_ref, right_ref, [(r + 1) * wide + c + 1 for r in range(ct) for c in range(cc)])

    def finish(jobs, places, add):
        for sums, (slot, index) in zip(pushes(left_ref, sum_ref, right_ref, jobs), places):
            start = slot * 8 if isinstance(slot, int) else pl.multiple_of(slot * 8, 8)
            store_rows(out_ref, moment(state_ref[pl.ds(start, 8), :], sums), index, add)

    if ct != 2:
        out_ref[...] = jnp.zeros_like(out_ref)

    def several(step, carry):
        jobs, places = [], []
        for k in range(columns):
            c = step * columns + k
            for r, rr in ((0, 0), (ct - 1, ct + 1)):
                jobs.append((r * cc + c, [rr * wide + c + d for d in range(3)]))
                places.append(((r + 1) * wide + c + 1, r * cc + c))
        finish(jobs, places, ct != 2)
        return carry

    lax.fori_loop(0, cc // columns, several, 0)
    jobs, places = [], []
    for r in range(ct):
        near = range(max(r - 1, 0), min(r + 2, ct))
        for c, p in ((0, 0), (cc - 1, cc + 1)):
            jobs.append((r * cc + c, [(q + 1) * wide + p for q in near]))
            places.append(((r + 1) * wide + c + 1, r * cc + c))
    finish(jobs, places, True)


def face_kernel(second, cc, crosses, s_ref, index_ref, offset_ref, velocity_ref, all_ref, *rest):
    if second:
        force_ref, before_ref, *rest = rest
    part_ref, react_ref, halo_ref, state_ref, face_ref = rest
    devices, _, cells, _ = all_ref.shape
    count = offset_ref.shape[0]
    pack(cc, crosses, s_ref, force_ref if second else all_ref, halo_ref)

    def spread(device, carry):
        base = pl.multiple_of(device * cells * 8, 8)
        for axis in range(3):
            x, v = all_ref[device, axis], all_ref[device, axis + 3]
            if second:
                x, v = advanced(x, v, force_ref[device, axis], axis)
            state_ref[pl.ds(base + axis, cells, stride=8), :] = x
            state_ref[pl.ds(base + 3 + axis, cells, stride=8), :] = v
            part_ref[device, axis] = jnp.zeros_like(x)
        return carry

    lax.fori_loop(0, devices, spread, 0)
    for axis in range(3):
        y, w = offset_ref[:, axis, :], velocity_ref[:, axis, :]
        if second:
            y = y + time_step * w
        face_ref[pl.ds(axis, count, stride=8), :] = y
        face_ref[pl.ds(3 + axis, count, stride=8), :] = w

    group = next(n for n in (faces_at_once, 4, 2, 1) if count % n == 0)

    def several(g, carry):
        blocks, states, faces, rights, lefts, sums, back_sums = [], [], [], [], [], [], []
        for k in range(group):
            f = g * group + k
            block = index_ref[f]
            state = state_ref[pl.ds(pl.multiple_of(block * 8, 8), 8), :]
            face = face_ref[pl.ds(pl.multiple_of(f * 8, 8), 8), :]
            pieces, row = features(state, soften * soften)
            face_pieces, _ = features(face, 0.0)
            blocks.append(block)
            states.append(state)
            faces.append(face)
            lefts.append(left_side(face_pieces, row))
            rights.append(right_side(pieces, row))
            sums.append(sum_side(face_pieces))
            back_sums.append(sum_side(pieces))
        waiting, done = [], []
        for n in range(group + ahead):
            if n < group:
                waiting.append(dot(lefts[n], rights[n]))
            if n >= ahead and n - ahead < group:
                k = n - ahead
                high, low = pair_weights(waiting[k], radius + face_radius)
                done.append(
                    (
                        dot(sums[k], jnp.concatenate([high, low], axis=0)),
                        dot(back_sums[k], jnp.concatenate([high, low], axis=1), ((1,), (1,))),
                    )
                )
        for k in range(group):
            onto, back = moment(states[k], done[k][0]), moment(faces[k], done[k][1])
            back = (time_step * damping * back)[0:3]
            react_ref[g * group + k] = before_ref[g * group + k] + back if second else back
            device, cell = blocks[k] // cells, blocks[k] % cells
            for axis in range(3):
                line = part_ref[device, axis, pl.ds(cell, 1), :]
                part_ref[device, axis, pl.ds(cell, 1), :] = line + damping * onto[axis : axis + 1]
        return carry

    lax.fori_loop(0, count // group, several, 0)


def pack(cc, crosses, s_ref, all_ref, out_ref):
    fields = all_ref.shape[1]
    c_index, first, row = s_ref[0], s_ref[1] * crosses, s_ref[8]
    for p in range(cc + 2):
        shift = -1 if p == 0 else (1 if p == cc + 1 else 0)
        device = first + jnp.clip(c_index + shift, 0, crosses - 1)
        cell = row * cc + (p - 1) % cc
        for f in range(fields):
            out_ref[pl.ds(p * fields + f, 1), :] = all_ref[device, f, pl.ds(cell, 1), :]


def call(kernel, name, args, scalars, outs, scratch, flops):
    specs = [pl.BlockSpec(memory_space=SMEM)] * scalars
    specs += [pl.BlockSpec(memory_space=VMEM)] * (len(args) - scalars)
    return pl.pallas_call(
        kernel,
        name=name,
        out_shape=[jax.ShapeDtypeStruct(s, f32) for s in outs],
        in_specs=specs,
        out_specs=[pl.BlockSpec(memory_space=VMEM)] * len(outs),
        scratch_shapes=scratch,
        cost_estimate=pl.CostEstimate(flops=flops, transcendentals=0, bytes_accessed=0),
    )(*args)


def body(
    particle_offset,
    particle_velocity,
    cell_count,
    face_offset,
    face_velocity,
    face_route,
    face_cell,
):
    _, ct, cc, slots = particle_offset.shape
    cells = ct * cc
    own_faces, _, faces = face_offset.shape
    vehicles, tracks, crosses = [lax.axis_size(a) for a in ("vehicle", "track", "cross")]
    vehicle, track, cross = [lax.axis_index(a) for a in ("vehicle", "track", "cross")]
    pair = tracks == 2
    wide = cc + 2
    grid_slots = (ct + 2) * wide
    ring_slots = [
        VMEM((grid_slots * 8, slots), f32),
        VMEM((grid_slots, slots, 80), bf16),
        VMEM((grid_slots, 32, 2 * slots), bf16),
        VMEM((cells, 80, 2 * slots), bf16),
    ]

    x = particle_offset.reshape(3, cells, slots)
    v = particle_velocity.reshape(3, cells, slots)
    live = (
        lax.broadcasted_iota(jnp.int32, (cells, slots), 1) < cell_count.reshape(cells)[:, None]
    )
    first = lax.broadcasted_iota(jnp.int32, (3, 1, 1), 0) == 0

    def marked(x):
        return jnp.where(first & ~live[None], far, x)

    def place(t):
        return jnp.bitwise_xor(t, track) if pair else t

    low, high = track > 0, track < tracks - 1
    target = face_route[:, 0]
    index = (place(target // crosses) * crosses + target % crosses) * cells + face_cell
    scalars = jnp.stack(
        [
            cross,
            place(track),
            low,
            place(jnp.maximum(track - 1, 0)),
            low | (vehicle > 0),
            high,
            place(jnp.minimum(track + 1, tracks - 1)),
            high | (vehicle < vehicles - 1),
            jnp.where(high, 0, ct - 1),
        ]
    ).astype(jnp.int32)
    swap = [(0, 1), (1, 0)]
    travel = []
    for e in range(vehicles - 1):
        last, following = e * tracks + tracks - 1, (e + 1) * tracks
        travel += [(last, following), (following, last)]

    def gather_cross(a):
        spread = jnp.broadcast_to(a[None], (crosses,) + a.shape)
        return lax.all_to_all(spread, "cross", split_axis=0, concat_axis=0, tiled=True)

    def gather_track(a):
        if pair:
            return jnp.concatenate([a, lax.ppermute(a, "track", swap)], axis=0)
        return lax.all_gather(a, "track", axis=0, tiled=True)

    def scatter_force(part):
        part = part.reshape(tracks, crosses, 3, cells, slots)
        if pair:
            part = part[0] + lax.ppermute(part[1], "track", swap)
        else:
            part = jnp.sum(lax.all_to_all(part, "track", 0, 0, tiled=True), axis=0)
        return lax.all_to_all(part, "cross", 0, 0, tiled=True)

    fall = jnp.array(falls, f32)[:, None, None]
    reaction = None
    everyone = beyond = None
    force = None
    for substep in range(2):
        second = substep == 1
        own = marked(x)
        mine = gather_cross(force if second else jnp.concatenate([own, v], axis=0))
        inner = call(
            functools.partial(inner_kernel, ct, cc),
            "inner",
            [own, v],
            0,
            [(3, cells, slots)],
            ring_slots,
            4 * 10**9,
        )[0]
        mine, inner = lax.optimization_barrier((mine, inner))
        group = gather_track(mine)
        if second:
            extra, before = [group], [reaction]
        else:
            everyone, extra, before = group, [], []
        part, reaction, packed = call(
            functools.partial(face_kernel, second, cc, crosses),
            "faces",
            [scalars, index, face_offset, face_velocity, everyone] + extra + before,
            2,
            [
                (tracks * crosses, 3, cells, slots),
                (own_faces, 3, faces),
                (wide * group.shape[1], slots),
            ],
            [
                VMEM((tracks * crosses * cells * 8, slots), f32),
                VMEM((own_faces * 8, faces), f32),
            ],
            4 * 10**9,
        )
        across = lax.ppermute(packed, ("vehicle", "track"), travel)
        if second:
            halo_extra = [across]
        else:
            beyond, halo_extra = across, []
        outer = call(
            functools.partial(outer_kernel, ct, cc, crosses, second),
            "outer",
            [scalars, own, v, everyone, beyond] + extra + halo_extra,
            1,
            [(3, cells, slots)],
            ring_slots,
            4 * 10**9,
        )[0]
        returned, outer = lax.optimization_barrier((scatter_force(part), outer))
        force = jnp.where(live[None], inner + outer, 0.0) + jnp.sum(returned, axis=0)
        v = v + time_step * (force + fall)
        x = x + time_step * v
    shape = particle_offset.shape
    return (x.reshape(shape), v.reshape(shape), reaction)


def solution(mesh):
    in_specs = (
        P(None, ("vehicle", "track"), "cross", None),
        P(None, ("vehicle", "track"), "cross", None),
        P(("vehicle", "track"), "cross"),
        P(("vehicle", "track", "cross"), None, None),
        P(("vehicle", "track", "cross"), None, None),
        P(("vehicle", "track", "cross"), None),
        P(("vehicle", "track", "cross")),
    )
    out_specs = (
        P(None, ("vehicle", "track"), "cross", None),
        P(None, ("vehicle", "track"), "cross", None),
        P(("vehicle", "track", "cross"), None, None),
    )
    return jax.shard_map(body, mesh=mesh, in_specs=in_specs, out_specs=out_specs, check_vma=False)
```

```python
import functools

import jax
import jax.numpy as jnp
from jax import lax
from jax.experimental import pallas as pl
from jax.experimental.pallas import tpu as pltpu
from jax.sharding import PartitionSpec as P

radius = 0.1
face_radius = 0.15
stiffness = 100.0
damping = 40.0
soften = 0.05
time_step = 0.02
gravity = 9.81

far = 1000.0
ahead = 8
columns = 4
faces_at_once = 16
scratch_bytes = 20 * 2**20
f32 = jnp.float32
bf16 = jnp.bfloat16
falls = (0.0, 0.0, -gravity)
VMEM = pltpu.VMEM
SMEM = pltpu.SMEM
VMEM_SPACE = pltpu.MemorySpace.VMEM


def split3(a):
    high = a.astype(bf16).astype(f32)
    rest = a - high
    mid = rest.astype(bf16).astype(f32)
    return high, mid, rest - mid


def features(state, eps):
    row = lax.broadcasted_iota(jnp.int32, state.shape, 0)
    turned = pltpu.roll(state, 5, 0)
    square = jnp.sum(jnp.where(row < 3, state * state, 0.0), axis=0, keepdims=True) + eps
    cross = jnp.sum(jnp.where(row < 3, state * turned, 0.0), axis=0, keepdims=True)
    full = jnp.where(row == 6, square, jnp.where(row == 7, cross, state))
    return split3(full), row


def left_side(pieces, row):
    p1, p2, p3 = pieces
    ones = jnp.where(row >= 6, 1.0, 0.0)
    zero = jnp.zeros_like(p1)
    stack = jnp.concatenate([p1, p1, p2, p1, p3, p2, ones, ones, ones, zero], axis=0)
    return jnp.transpose(stack).astype(bf16)


def right_side(pieces, row):
    def for_square(p, first):
        return jnp.where(row < 3, -2.0 * p, jnp.where(row == 6, 1.0 if first else 0.0, 0.0))

    def for_closing(p, first):
        swapped = jnp.where(row < 3, pltpu.roll(p, 5, 0), pltpu.roll(p, 3, 0))
        return jnp.where(row < 6, -swapped, jnp.where(row == 7, 1.0 if first else 0.0, 0.0))

    halves = []
    for side, keep in ((for_square, 6), (for_closing, 7)):
        b1, b2, b3 = [side(p, k == 0) for k, p in enumerate(pieces)]
        q = [jnp.where(row == keep, p, 0.0) for p in pieces]
        halves.append(jnp.concatenate([b1, b2, b1, b3, b1, b2] + q + [jnp.zeros_like(b1)], axis=0))
    return jnp.concatenate(halves, axis=1).astype(bf16)


def sum_side(pieces):
    p1, p2, p3 = pieces
    stack = jnp.concatenate([p1, p2, p3, jnp.ones_like(p1)], axis=0).astype(bf16)
    return jnp.concatenate([stack, stack], axis=1)


def pair_weights(product, reach):
    n = product.shape[1] // 2
    square = jnp.maximum(product[:, :n], soften * soften * 0.5)
    inverse = lax.rsqrt(square)
    weight = jnp.maximum(reach * inverse - 1.0, 0.0) * (
        stiffness / damping - product[:, n:] * inverse
    )
    high = weight.astype(bf16)
    low = (weight - high.astype(f32)).astype(bf16)
    return high, low


def dot(a, b, contract=((1,), (0,))):
    return lax.dot_general(a, b, (contract, ((), ())), preferred_element_type=f32)


def moment(state, sums):
    total = sums[0:8] + sums[8:16] + sums[16:24]
    return state * sums[24:25] - total


def advanced(x, v, force, axis):
    v = v + time_step * (force + falls[axis])
    return x + time_step * v, v


def put_own(state_ref, x_ref, v_ref, ct, cc):
    cells = lax.broadcasted_iota(jnp.int32, (cc, 128), 0).astype(f32)
    for r in range(ct):
        base = ((r + 1) * (cc + 2) + 1) * 8
        for axis in range(3):
            x = x_ref[axis, pl.ds(r * cc, cc), :]
            if axis == 0:
                x = x + (r + 1 - (ct + 1) / 2)
            if axis == 1:
                x = x + (cells + (1 - (cc + 1) / 2))
            state_ref[pl.ds(base + axis, cc, stride=8), :] = x
            state_ref[pl.ds(base + 3 + axis, cc, stride=8), :] = v_ref[axis, pl.ds(r * cc, cc), :]


def put_dead(state_ref, slot):
    row = lax.broadcasted_iota(jnp.int32, (8, 128), 0)
    state_ref[pl.ds(slot * 8, 8), :] = jnp.where(row == 0, far, 0.0)


def build_left(state_ref, left_ref, sum_ref, slots):
    for slot in slots:
        pieces, row = features(state_ref[pl.ds(slot * 8, 8), :], 0.0)
        left_ref[slot] = left_side(pieces, row)
        sum_ref[slot] = sum_side(pieces)


def build_right(state_ref, right_ref, slots):
    for k, slot in enumerate(slots):
        pieces, row = features(state_ref[pl.ds(slot * 8, 8), :], soften * soften)
        right_ref[k] = right_side(pieces, row)


def pushes(left_ref, sum_ref, right_ref, jobs):
    todo = [(k, block, slot) for k, (block, others) in enumerate(jobs) for slot in others]
    totals = [None] * len(jobs)
    waiting = []
    for n in range(len(todo) + ahead):
        if n < len(todo):
            k, block, slot = todo[n]
            waiting.append((k, slot, dot(left_ref[slot], right_ref[block])))
        if n >= ahead:
            k, slot, product = waiting.pop(0)
            high, low = pair_weights(product, 2.0 * radius)
            part = dot(sum_ref[slot], jnp.concatenate([high, low], axis=0))
            totals[k] = part if totals[k] is None else totals[k] + part
    return totals


def store_rows(out_ref, values, index, add):
    for axis in range(3):
        line = damping * values[axis : axis + 1]
        if add:
            line = line + out_ref[axis, pl.ds(index, 1), :]
        out_ref[axis, pl.ds(index, 1), :] = line


def inner_kernel(ct, cc, x_ref, v_ref, out_ref, state_ref, left_ref, sum_ref, right_ref):
    wide = cc + 2
    own = [(r + 1) * wide + c + 1 for r in range(ct) for c in range(cc)]
    ends = [(r + 1) * wide + c for r in range(ct) for c in (0, cc + 1)]
    put_own(state_ref, x_ref, v_ref, ct, cc)
    for slot in ends:
        put_dead(state_ref, slot)
    build_left(state_ref, left_ref, sum_ref, own + ends)
    build_right(state_ref, right_ref, own)

    def several(step, carry):
        jobs, places = [], []
        for k in range(columns):
            c = step * columns + k
            for r in range(ct):
                near = range(max(r - 1, 0), min(r + 2, ct))
                jobs.append((r * cc + c, [(q + 1) * wide + c + d for q in near for d in range(3)]))
                places.append(((r + 1) * wide + c + 1, r * cc + c))
        for sums, (slot, index) in zip(pushes(left_ref, sum_ref, right_ref, jobs), places):
            state = state_ref[pl.ds(pl.multiple_of(slot * 8, 8), 8), :]
            store_rows(out_ref, moment(state, sums), index, False)
        return carry

    lax.fori_loop(0, cc // columns, several, 0)


class Gathered:
    def __init__(self, refs, crosses, track):
        self.refs, self.crosses, self.track = refs, crosses, track

    def line(self, shift, device, field, cell):
        if len(self.refs) == 2:
            return self.refs[0 if shift == 0 else 1][device, field, pl.ds(cell, 1), :]
        tracks = self.refs[0].shape[0] // self.crosses
        track = jnp.clip(self.track + shift, 0, tracks - 1)
        return self.refs[0][track * self.crosses + device, field, pl.ds(cell, 1), :]


def outer_kernel(ct, cc, crosses, nrefs, second, x_ref, v_ref, *rest):
    track, c_index = lax.axis_index("track"), lax.axis_index("cross")
    vehicle = lax.axis_index("vehicle")
    vehicles, tracks = lax.axis_size("vehicle"), lax.axis_size("track")
    gathered = [Gathered(rest[:nrefs], crosses, track)]
    halos = [rest[nrefs]]
    rest = rest[nrefs + 1 :]
    if second:
        gathered.append(Gathered(rest[:nrefs], crosses, track))
        halos.append(rest[nrefs])
        rest = rest[nrefs + 1 :]
    out_ref, state_ref, left_ref, sum_ref, right_ref = rest
    wide = cc + 2
    has_low = c_index > 0
    has_high = c_index < crosses - 1
    put_own(state_ref, x_ref, v_ref, ct, cc)

    def place(slot, rr, p, load, ok):
        for axis in range(3):
            x, v = load(axis, 6, 0), load(axis + 3, 6, 0)
            if second:
                x, v = advanced(x, v, load(axis, 3, 1), axis)
            if axis == 0:
                x = x + (rr - (ct + 1) / 2)
                x = jnp.where(ok, x, far)
            if axis == 1:
                x = jnp.where(ok, x + (p - (cc + 1) / 2), 0.0)
            state_ref[pl.ds(slot * 8 + axis, 1), :] = x
            state_ref[pl.ds(slot * 8 + 3 + axis, 1), :] = jnp.where(ok, v, 0.0)

    def from_all(shift, row, p):
        step = -1 if p == 0 else (1 if p == cc + 1 else 0)
        device = jnp.clip(c_index + step, 0, crosses - 1)
        cell = row * cc + (p - 1) % cc
        return lambda f, n, k: gathered[k].line(shift, device, f, cell)

    def from_halo(p):
        return lambda f, n, k: halos[k][pl.ds(p * n + f, 1), :]

    for rr, shift, row in ((0, -1, ct - 1), (ct + 1, 1, 0)):
        if shift < 0:
            inside, exists = track > 0, (track > 0) | (vehicle > 0)
        else:
            inside = track < tracks - 1
            exists = inside | (vehicle < vehicles - 1)
        for p in range(wide):
            a, b = from_all(shift, row, p), from_halo(p)

            def load(f, n, k, a=a, b=b):
                return jnp.where(inside, a(f, n, k), b(f, n, k))

            ok = exists
            if p == 0:
                ok = jnp.logical_and(ok, has_low)
            if p == cc + 1:
                ok = jnp.logical_and(ok, has_high)
            place(rr * wide + p, rr, p, load, ok)
    for r in range(ct):
        place((r + 1) * wide, r + 1, 0, from_all(0, r, 0), has_low)
        place((r + 1) * wide + cc + 1, r + 1, cc + 1, from_all(0, r, cc + 1), has_high)
    ring = [rr * wide + p for rr in (0, ct + 1) for p in range(wide)]
    ring += [(r + 1) * wide + p for r in range(ct) for p in (0, cc + 1)]
    build_left(state_ref, left_ref, sum_ref, ring)
    build_right(state_ref, right_ref, [(r + 1) * wide + c + 1 for r in range(ct) for c in range(cc)])

    def finish(jobs, places, add):
        for sums, (slot, index) in zip(pushes(left_ref, sum_ref, right_ref, jobs), places):
            start = slot * 8 if isinstance(slot, int) else pl.multiple_of(slot * 8, 8)
            store_rows(out_ref, moment(state_ref[pl.ds(start, 8), :], sums), index, add)

    if ct != 2:
        out_ref[...] = jnp.zeros_like(out_ref)

    def several(step, carry):
        jobs, places = [], []
        for k in range(columns):
            c = step * columns + k
            for r, rr in ((0, 0), (ct - 1, ct + 1)):
                jobs.append((r * cc + c, [rr * wide + c + d for d in range(3)]))
                places.append(((r + 1) * wide + c + 1, r * cc + c))
        finish(jobs, places, ct != 2)
        return carry

    lax.fori_loop(0, cc // columns, several, 0)
    jobs, places = [], []
    for r in range(ct):
        near = range(max(r - 1, 0), min(r + 2, ct))
        for c, p in ((0, 0), (cc - 1, cc + 1)):
            jobs.append((r * cc + c, [(q + 1) * wide + p for q in near]))
            places.append(((r + 1) * wide + c + 1, r * cc + c))
    finish(jobs, places, True)


def face_kernel(second, ct, cc, crosses, nrefs, route_ref, cell_ref, offset_ref, velocity_ref, *rest):
    all_refs, rest = rest[:nrefs], rest[nrefs:]
    if second:
        force_refs, before_ref, rest = rest[:nrefs], rest[nrefs], rest[nrefs + 1 :]
    part_refs, (react_ref, halo_ref, state_ref, face_ref, part_ref) = rest[:nrefs], rest[nrefs:]
    devices, _, cells, _ = all_refs[0].shape
    count = offset_ref.shape[1]
    track = lax.axis_index("track")
    pack(ct, cc, crosses, track, force_refs if second else all_refs, halo_ref)

    for k in range(nrefs):

        def spread(device, carry, k=k):
            base = pl.multiple_of((k * devices + device) * cells * 8, 8)
            for axis in range(3):
                x, v = all_refs[k][device, axis], all_refs[k][device, axis + 3]
                if second:
                    x, v = advanced(x, v, force_refs[k][device, axis], axis)
                state_ref[pl.ds(base + axis, cells, stride=8), :] = x
                state_ref[pl.ds(base + 3 + axis, cells, stride=8), :] = v
                part_ref[k * devices + device, axis] = jnp.zeros_like(x)
            return carry

        lax.fori_loop(0, devices, spread, 0, unroll=min(devices, 4))
    for axis in range(3):
        y, w = offset_ref[axis], velocity_ref[axis]
        if second:
            y = y + time_step * w
        face_ref[pl.ds(axis, count, stride=8), :] = y
        face_ref[pl.ds(3 + axis, count, stride=8), :] = w

    def block_of(f):
        target = route_ref[f]
        where, across = lax.div(target, crosses), lax.rem(target, crosses)
        if nrefs == 2:
            where = jnp.bitwise_xor(where, track)
        return where * crosses + across, cell_ref[f]

    group = next(n for n in (faces_at_once, 4, 2, 1) if count % n == 0)

    def several(g, carry):
        blocks, states, faces, rights, lefts, sums, back_sums = [], [], [], [], [], [], []
        for k in range(group):
            f = g * group + k
            block = block_of(f)
            place = (block[0] * cells + block[1]) * 8
            state = state_ref[pl.ds(pl.multiple_of(place, 8), 8), :]
            face = face_ref[pl.ds(pl.multiple_of(f * 8, 8), 8), :]
            pieces, row = features(state, soften * soften)
            face_pieces, _ = features(face, 0.0)
            blocks.append(block)
            states.append(state)
            faces.append(face)
            lefts.append(left_side(face_pieces, row))
            rights.append(right_side(pieces, row))
            sums.append(sum_side(face_pieces))
            back_sums.append(sum_side(pieces))
        waiting, done = [], []
        for n in range(group + ahead):
            if n < group:
                waiting.append(dot(lefts[n], rights[n]))
            if n >= ahead and n - ahead < group:
                k = n - ahead
                high, low = pair_weights(waiting[k], radius + face_radius)
                done.append(
                    (
                        dot(sums[k], jnp.concatenate([high, low], axis=0)),
                        dot(back_sums[k], jnp.concatenate([high, low], axis=1), ((1,), (1,))),
                    )
                )
        for k in range(group):
            onto, back = moment(states[k], done[k][0]), moment(faces[k], done[k][1])
            device, cell = blocks[k]
            for axis in range(3):
                line = time_step * damping * back[axis : axis + 1]
                at = pl.ds(g * group + k, 1)
                if second:
                    line = line + before_ref[axis, at, :]
                react_ref[axis, at, :] = line
                line = part_ref[device, axis, pl.ds(cell, 1), :]
                part_ref[device, axis, pl.ds(cell, 1), :] = line + damping * onto[axis : axis + 1]
        return carry

    lax.fori_loop(0, count // group, several, 0)
    for k in range(nrefs):
        part_refs[k][...] = part_ref[pl.ds(k * devices, devices)]


def pack(ct, cc, crosses, track, refs, out_ref):
    gathered = Gathered(refs, crosses, track)
    fields = refs[0].shape[1]
    c_index = lax.axis_index("cross")
    row = jnp.where(track < lax.axis_size("track") - 1, 0, ct - 1)
    for p in range(cc + 2):
        step = -1 if p == 0 else (1 if p == cc + 1 else 0)
        device = jnp.clip(c_index + step, 0, crosses - 1)
        cell = row * cc + (p - 1) % cc
        for f in range(fields):
            out_ref[pl.ds(p * fields + f, 1), :] = gathered.line(0, device, f, cell)


def first_kernel(count_ref, x_ref, v_ref, own_ref, live_ref, spread_ref):
    ct, cc = count_ref.shape
    shape = live_ref.shape
    row = lax.broadcasted_iota(jnp.int32, shape, 0)
    lane = lax.broadcasted_iota(jnp.int32, shape, 1)
    count = jnp.zeros(shape, jnp.int32)
    for cell in range(ct * cc):
        count = jnp.where(row == cell, count_ref[cell // cc, cell % cc], count)
    live = lane < count
    live_ref[...] = jnp.where(live, 1.0, 0.0)
    for axis in range(3):
        x, v = x_ref[axis], v_ref[axis]
        if axis == 0:
            x = jnp.where(live, x, far)
        own_ref[axis] = x
        for k in range(spread_ref.shape[0]):
            spread_ref[k, axis] = x
            spread_ref[k, axis + 3] = v


def update_kernel(second, live_ref, x_ref, v_ref, inner_ref, outer_ref, back_ref, *outs):
    live = live_ref[...] > 0.5
    for axis in range(3):
        force = jnp.where(live, inner_ref[axis] + outer_ref[axis], 0.0)
        for k in range(back_ref.shape[0]):
            force = force + back_ref[k, axis]
        x, v = advanced(x_ref[axis], v_ref[axis], force, axis)
        outs[0][axis] = x
        outs[1][axis] = v
        if not second:
            outs[2][axis] = jnp.where(live, x, far) if axis == 0 else x
            for k in range(back_ref.shape[0]):
                outs[3][k, axis] = force


def call(kernel, name, scalars, args, outs, scratch, flops, keep=True):
    specs = [pl.BlockSpec(memory_space=SMEM)] * len(scalars)
    specs += [pl.BlockSpec(memory_space=VMEM)] * len(args)
    shapes = [VMEM(s, f32) if keep else jax.ShapeDtypeStruct(s, f32) for s in outs]
    return pl.pallas_call(
        kernel,
        name=name,
        out_shape=shapes,
        in_specs=specs,
        out_specs=[pl.BlockSpec(memory_space=VMEM)] * len(outs),
        scratch_shapes=scratch,
        compiler_params=pltpu.CompilerParams(vmem_limit_bytes=scratch_bytes),
        cost_estimate=pl.CostEstimate(flops=flops, transcendentals=0, bytes_accessed=0),
    )(*scalars, *[pltpu.with_memory_space_constraint(a, VMEM_SPACE) for a in args])


def body(
    particle_offset,
    particle_velocity,
    cell_count,
    face_offset,
    face_velocity,
    face_route,
    face_cell,
):
    _, ct, cc, slots = particle_offset.shape
    cells = ct * cc
    own_faces, _, faces = face_offset.shape
    vehicles, tracks, crosses = [lax.axis_size(a) for a in ("vehicle", "track", "cross")]
    pair = tracks == 2
    nrefs = 2 if pair else 1
    devices = tracks * crosses
    wide = cc + 2
    grid_slots = (ct + 2) * wide
    ring_slots = [
        VMEM((grid_slots * 8, slots), f32),
        VMEM((grid_slots, slots, 80), bf16),
        VMEM((grid_slots, 32, 2 * slots), bf16),
        VMEM((cells, 80, 2 * slots), bf16),
    ]
    block = (3, cells, slots)
    swap = [(0, 1), (1, 0)]
    travel = []
    for e in range(vehicles - 1):
        last, following = e * tracks + tracks - 1, (e + 1) * tracks
        travel += [(last, following), (following, last)]

    def exchange(a):
        return lax.all_to_all(a, "cross", split_axis=0, concat_axis=0, tiled=True)

    def gather_track(a):
        if pair:
            return [a, lax.ppermute(a, "track", swap)]
        return [lax.all_gather(a, "track", axis=0, tiled=True)]

    def sum_track(parts):
        if pair:
            return parts[0] + lax.ppermute(parts[1], "track", swap)
        part = parts[0].reshape(tracks, crosses, 3, cells, slots)
        return jnp.sum(lax.all_to_all(part, "track", 0, 0, tiled=True), axis=0)

    x = particle_offset.reshape(block)
    v = particle_velocity.reshape(block)
    offset_rows = jnp.transpose(face_offset, (1, 0, 2))
    velocity_rows = jnp.transpose(face_velocity, (1, 0, 2))
    own, live, spread = call(
        first_kernel,
        "first",
        [cell_count],
        [x, v],
        [block, (cells, slots), (crosses, 6, cells, slots)],
        [],
        10**6,
    )
    reaction = everyone = beyond = None
    for substep in range(2):
        second = substep == 1
        mine = exchange(spread)
        inner = call(
            functools.partial(inner_kernel, ct, cc), "inner", [], [own, v], [block], ring_slots, 10**9
        )[0]
        mine, inner = lax.optimization_barrier((mine, inner))
        group = gather_track(mine)
        if second:
            extra, before = group, [reaction]
        else:
            everyone, extra, before = group, [], []
        *parts, reaction, packed = call(
            functools.partial(face_kernel, second, ct, cc, crosses, nrefs),
            "faces",
            [face_route.reshape(own_faces), face_cell],
            [offset_rows, velocity_rows] + everyone + extra + before,
            [(devices // nrefs, 3, cells, slots)] * nrefs
            + [(3, own_faces, faces), (wide * group[0].shape[1], slots)],
            [
                VMEM((devices * cells * 8, slots), f32),
                VMEM((own_faces * 8, faces), f32),
                VMEM((devices, 3, cells, slots), f32),
            ],
            4 * 10**9,
        )
        across = lax.ppermute(packed, ("vehicle", "track"), travel)
        if second:
            halo_extra = [across]
        else:
            beyond, halo_extra = across, []
        outer = call(
            functools.partial(outer_kernel, ct, cc, crosses, nrefs, second),
            "outer",
            [],
            [own, v] + everyone + [beyond] + extra + halo_extra,
            [block],
            ring_slots,
            10**9,
        )[0]
        returned, outer = lax.optimization_barrier((exchange(sum_track(parts)), outer))
        new = call(
            functools.partial(update_kernel, second),
            "update",
            [],
            [live, x, v, inner, outer, returned],
            [block, block] if second else [block, block, block, (crosses, 3, cells, slots)],
            [],
            10**6,
            not second,
        )
        x, v = new[:2]
        if not second:
            own, spread = new[2:]
    shape = particle_offset.shape
    return (x.reshape(shape), v.reshape(shape), jnp.transpose(reaction, (1, 0, 2)))


def solution(mesh):
    in_specs = (
        P(None, ("vehicle", "track"), "cross", None),
        P(None, ("vehicle", "track"), "cross", None),
        P(("vehicle", "track"), "cross"),
        P(("vehicle", "track", "cross"), None, None),
        P(("vehicle", "track", "cross"), None, None),
        P(("vehicle", "track", "cross"), None),
        P(("vehicle", "track", "cross")),
    )
    out_specs = (
        P(None, ("vehicle", "track"), "cross", None),
        P(None, ("vehicle", "track"), "cross", None),
        P(("vehicle", "track", "cross"), None, None),
    )
    return jax.shard_map(body, mesh=mesh, in_specs=in_specs, out_specs=out_specs, check_vma=False)
```

```python
import functools

import jax
import jax.numpy as jnp
from jax import lax
from jax.experimental import pallas as pl
from jax.experimental.pallas import tpu as pltpu
from jax.sharding import PartitionSpec as P

radius = 0.1
face_radius = 0.15
stiffness = 100.0
damping = 40.0
soften = 0.05
time_step = 0.02
gravity = 9.81

far = 1000.0
ahead = 8
columns = 4
faces_at_once = 16
scratch_bytes = 20 * 2**20
f32 = jnp.float32
bf16 = jnp.bfloat16
falls = (0.0, 0.0, -gravity)
VMEM = pltpu.VMEM
SMEM = pltpu.SMEM
VMEM_SPACE = pltpu.MemorySpace.VMEM


def split3(a):
    high = a.astype(bf16).astype(f32)
    rest = a - high
    mid = rest.astype(bf16).astype(f32)
    return high, mid, rest - mid


def features(state, eps):
    row = lax.broadcasted_iota(jnp.int32, state.shape, 0)
    turned = pltpu.roll(state, 5, 0)
    square = jnp.sum(jnp.where(row < 3, state * state, 0.0), axis=0, keepdims=True) + eps
    cross = jnp.sum(jnp.where(row < 3, state * turned, 0.0), axis=0, keepdims=True)
    full = jnp.where(row == 6, square, jnp.where(row == 7, cross, state))
    return split3(full), row


def left_side(pieces, row):
    p1, p2, p3 = pieces
    ones = jnp.where(row >= 6, 1.0, 0.0)
    zero = jnp.zeros_like(p1)
    stack = jnp.concatenate([p1, p1, p2, p1, p3, p2, ones, ones, ones, zero], axis=0)
    return jnp.transpose(stack).astype(bf16)


def right_side(pieces, row):
    def for_square(p, first):
        return jnp.where(row < 3, -2.0 * p, jnp.where(row == 6, 1.0 if first else 0.0, 0.0))

    def for_closing(p, first):
        swapped = jnp.where(row < 3, pltpu.roll(p, 5, 0), pltpu.roll(p, 3, 0))
        return jnp.where(row < 6, -swapped, jnp.where(row == 7, 1.0 if first else 0.0, 0.0))

    halves = []
    for side, keep in ((for_square, 6), (for_closing, 7)):
        b1, b2, b3 = [side(p, k == 0) for k, p in enumerate(pieces)]
        q = [jnp.where(row == keep, p, 0.0) for p in pieces]
        halves.append(jnp.concatenate([b1, b2, b1, b3, b1, b2] + q + [jnp.zeros_like(b1)], axis=0))
    return jnp.concatenate(halves, axis=1).astype(bf16)


def sum_side(pieces):
    p1, p2, p3 = pieces
    stack = jnp.concatenate([p1, p2, p3, jnp.ones_like(p1)], axis=0).astype(bf16)
    return jnp.concatenate([stack, stack], axis=1)


def pair_weights(product, reach):
    n = product.shape[1] // 2
    square = jnp.maximum(product[:, :n], soften * soften * 0.5)
    inverse = lax.rsqrt(square)
    weight = jnp.maximum(reach * inverse - 1.0, 0.0) * (
        stiffness / damping - product[:, n:] * inverse
    )
    high = weight.astype(bf16)
    low = (weight - high.astype(f32)).astype(bf16)
    return high, low


def dot(a, b, contract=((1,), (0,))):
    return lax.dot_general(a, b, (contract, ((), ())), preferred_element_type=f32)


def moment(state, sums):
    total = sums[0:8] + sums[8:16] + sums[16:24]
    return state * sums[24:25] - total


def advanced(x, v, force, axis):
    v = v + time_step * (force + falls[axis])
    return x + time_step * v, v


def put_own(state_ref, x_ref, v_ref, ct, cc):
    cells = lax.broadcasted_iota(jnp.int32, (cc, 128), 0).astype(f32)
    for r in range(ct):
        base = ((r + 1) * (cc + 2) + 1) * 8
        for axis in range(3):
            x = x_ref[axis, pl.ds(r * cc, cc), :]
            if axis == 0:
                x = x + (r + 1 - (ct + 1) / 2)
            if axis == 1:
                x = x + (cells + (1 - (cc + 1) / 2))
            state_ref[pl.ds(base + axis, cc, stride=8), :] = x
            state_ref[pl.ds(base + 3 + axis, cc, stride=8), :] = v_ref[axis, pl.ds(r * cc, cc), :]


def build_left(state_ref, left_ref, sum_ref, slots):
    for slot in slots:
        pieces, row = features(state_ref[pl.ds(slot * 8, 8), :], 0.0)
        left_ref[slot] = left_side(pieces, row)
        sum_ref[slot] = sum_side(pieces)


def build_right(state_ref, right_ref, slots):
    for k, slot in enumerate(slots):
        pieces, row = features(state_ref[pl.ds(slot * 8, 8), :], soften * soften)
        right_ref[k] = right_side(pieces, row)


def pushes(left_ref, sum_ref, right_ref, jobs):
    todo = [(k, block, slot) for k, (block, others) in enumerate(jobs) for slot in others]
    totals = [None] * len(jobs)
    waiting = []
    for n in range(len(todo) + ahead):
        if n < len(todo):
            k, block, slot = todo[n]
            waiting.append((k, slot, dot(left_ref[slot], right_ref[block])))
        if n >= ahead:
            k, slot, product = waiting.pop(0)
            high, low = pair_weights(product, 2.0 * radius)
            part = dot(sum_ref[slot], jnp.concatenate([high, low], axis=0))
            totals[k] = part if totals[k] is None else totals[k] + part
    return totals


def store_rows(out_ref, values, index, add):
    for axis in range(3):
        line = damping * values[axis : axis + 1]
        if add:
            line = line + out_ref[axis, pl.ds(index, 1), :]
        out_ref[axis, pl.ds(index, 1), :] = line


def inner_kernel(ct, cc, x_ref, v_ref, out_ref, right_ref, state_ref, left_ref, sum_ref):
    wide = cc + 2
    own = [(r + 1) * wide + c + 1 for r in range(ct) for c in range(cc)]
    put_own(state_ref, x_ref, v_ref, ct, cc)
    build_left(state_ref, left_ref, sum_ref, own)
    build_right(state_ref, right_ref, own)

    def finish(cells):
        jobs, places = [], []
        for c, steps in cells:
            for r in range(ct):
                near = range(max(r - 1, 0), min(r + 2, ct))
                jobs.append(
                    (r * cc + c, [(q + 1) * wide + c + 1 + d for q in near for d in steps])
                )
                places.append(((r + 1) * wide + c + 1, r * cc + c))
        for sums, (slot, index) in zip(pushes(left_ref, sum_ref, right_ref, jobs), places):
            start = slot * 8 if isinstance(slot, int) else pl.multiple_of(slot * 8, 8)
            store_rows(out_ref, moment(state_ref[pl.ds(start, 8), :], sums), index, False)

    def several(step, carry):
        finish([(1 + step * columns + k, (-1, 0, 1)) for k in range(columns)])
        return carry

    assert cc >= 2
    middle = cc - 2
    lax.fori_loop(0, middle // columns, several, 0)
    rest = [(c, (-1, 0, 1)) for c in range(1 + middle // columns * columns, cc - 1)]
    finish(rest + [(0, (0, 1)), (cc - 1, (-1, 0))])


class Gathered:
    def __init__(self, refs, crosses, track):
        self.refs, self.crosses, self.track = refs, crosses, track

    def line(self, shift, device, field, cell):
        if len(self.refs) == 2:
            return self.refs[0 if shift == 0 else 1][device, field, pl.ds(cell, 1), :]
        tracks = self.refs[0].shape[0] // self.crosses
        track = jnp.clip(self.track + shift, 0, tracks - 1)
        return self.refs[0][track * self.crosses + device, field, pl.ds(cell, 1), :]


def outer_kernel(ct, cc, crosses, nrefs, second, x_ref, v_ref, right_ref, *rest):
    track, c_index = lax.axis_index("track"), lax.axis_index("cross")
    vehicle = lax.axis_index("vehicle")
    vehicles, tracks = lax.axis_size("vehicle"), lax.axis_size("track")
    gathered = [Gathered(rest[:nrefs], crosses, track)]
    halos = [rest[nrefs]]
    rest = rest[nrefs + 1 :]
    if second:
        gathered.append(Gathered(rest[:1], crosses, track))
        halos.append(rest[1])
        rest = rest[2:]
    out_ref, state_ref, left_ref, sum_ref = rest
    wide = cc + 2
    has_low = c_index > 0
    has_high = c_index < crosses - 1
    put_own(state_ref, x_ref, v_ref, ct, cc)

    def place(slot, rr, p, load, ok):
        for axis in range(3):
            x, v = load(axis, 6, 0), load(axis + 3, 6, 0)
            if second:
                x, v = advanced(x, v, load(axis, 3, 1), axis)
            if axis == 0:
                x = x + (rr - (ct + 1) / 2)
                x = jnp.where(ok, x, far)
            if axis == 1:
                x = jnp.where(ok, x + (p - (cc + 1) / 2), 0.0)
            state_ref[pl.ds(slot * 8 + axis, 1), :] = x
            state_ref[pl.ds(slot * 8 + 3 + axis, 1), :] = jnp.where(ok, v, 0.0)

    def from_all(shift, row, p):
        step = -1 if p == 0 else (1 if p == cc + 1 else 0)
        device = jnp.clip(c_index + step, 0, crosses - 1)
        cell = row * cc + (p - 1) % cc
        return lambda f, n, k: gathered[k].line(shift, device, f, cell)

    def from_halo(p):
        return lambda f, n, k: halos[k][pl.ds(p * n + f, 1), :]

    for rr, shift, row in ((0, -1, ct - 1), (ct + 1, 1, 0)):
        if shift < 0:
            inside, exists = track > 0, (track > 0) | (vehicle > 0)
        else:
            inside = track < tracks - 1
            exists = inside | (vehicle < vehicles - 1)
        for p in range(wide):
            a, b = from_all(shift, row, p), from_halo(p)

            def load(f, n, k, a=a, b=b):
                return jnp.where(inside, a(f, n, k), b(f, n, k))

            ok = exists
            if p == 0:
                ok = jnp.logical_and(ok, has_low)
            if p == cc + 1:
                ok = jnp.logical_and(ok, has_high)
            place(rr * wide + p, rr, p, load, ok)
    for r in range(ct):
        place((r + 1) * wide, r + 1, 0, from_all(0, r, 0), has_low)
        place((r + 1) * wide + cc + 1, r + 1, cc + 1, from_all(0, r, cc + 1), has_high)
    ring = [rr * wide + p for rr in (0, ct + 1) for p in range(wide)]
    ring += [(r + 1) * wide + p for r in range(ct) for p in (0, cc + 1)]
    build_left(state_ref, left_ref, sum_ref, ring)

    def finish(jobs, places, add):
        for sums, (slot, index) in zip(pushes(left_ref, sum_ref, right_ref, jobs), places):
            start = slot * 8 if isinstance(slot, int) else pl.multiple_of(slot * 8, 8)
            store_rows(out_ref, moment(state_ref[pl.ds(start, 8), :], sums), index, add)

    if ct != 2:
        out_ref[...] = jnp.zeros_like(out_ref)

    def several(step, carry):
        jobs, places = [], []
        for k in range(columns):
            c = step * columns + k
            for r, rr in ((0, 0), (ct - 1, ct + 1)):
                jobs.append((r * cc + c, [rr * wide + c + d for d in range(3)]))
                places.append(((r + 1) * wide + c + 1, r * cc + c))
        finish(jobs, places, ct != 2)
        return carry

    lax.fori_loop(0, cc // columns, several, 0)
    jobs, places = [], []
    for r in range(ct):
        near = range(max(r - 1, 0), min(r + 2, ct))
        for c, p in ((0, 0), (cc - 1, cc + 1)):
            jobs.append((r * cc + c, [(q + 1) * wide + p for q in near]))
            places.append(((r + 1) * wide + c + 1, r * cc + c))
    finish(jobs, places, True)


def face_kernel(second, ct, cc, crosses, nrefs, route_from, cell_from, offset_ref, velocity_ref, *rest):
    all_refs, rest = rest[:nrefs], rest[nrefs:]
    if second:
        force_ref, before_ref, *rest = rest
    out_ref, react_ref, halo_ref, state_ref, face_ref, part_ref, route_ref, cell_ref, sems = rest
    copies = [
        pltpu.make_async_copy(route_from, route_ref, sems.at[0]),
        pltpu.make_async_copy(cell_from, cell_ref, sems.at[1]),
    ]
    for copy in copies:
        copy.start()
    devices, _, cells, _ = all_refs[0].shape
    count = offset_ref.shape[1]
    track = lax.axis_index("track")
    pack(ct, cc, crosses, track, [force_ref] if second else all_refs, halo_ref)

    starts = [jnp.bitwise_xor(k, track) * devices if nrefs == 2 else 0 for k in range(nrefs)]
    for k in range(nrefs):

        def spread(device, carry, k=k):
            base = pl.multiple_of((k * devices + device) * cells * 8, 8)
            for axis in range(3):
                x, v = all_refs[k][device, axis], all_refs[k][device, axis + 3]
                if second:
                    x, v = advanced(x, v, force_ref[starts[k] + device, axis], axis)
                state_ref[pl.ds(base + axis, cells, stride=8), :] = x
                state_ref[pl.ds(base + 3 + axis, cells, stride=8), :] = v
                part_ref[k * devices + device, axis] = jnp.zeros_like(x)
            return carry

        lax.fori_loop(0, devices, spread, 0, unroll=min(devices, 4))
    for axis in range(3):
        y, w = offset_ref[axis], velocity_ref[axis]
        if second:
            y = y + time_step * w
        face_ref[pl.ds(axis, count, stride=8), :] = y
        face_ref[pl.ds(3 + axis, count, stride=8), :] = w

    for copy in copies:
        copy.wait()

    def block_of(f):
        target = route_ref[f]
        where, across = lax.div(target, crosses), lax.rem(target, crosses)
        if nrefs == 2:
            where = jnp.bitwise_xor(where, track)
        return where * crosses + across, cell_ref[f]

    group = next(n for n in (faces_at_once, 4, 2, 1) if count % n == 0)

    def several(g, carry):
        blocks, states, faces, rights, lefts, sums, back_sums = [], [], [], [], [], [], []
        for k in range(group):
            f = g * group + k
            block = block_of(f)
            place = (block[0] * cells + block[1]) * 8
            state = state_ref[pl.ds(pl.multiple_of(place, 8), 8), :]
            face = face_ref[pl.ds(pl.multiple_of(f * 8, 8), 8), :]
            pieces, row = features(state, soften * soften)
            face_pieces, _ = features(face, 0.0)
            blocks.append(block)
            states.append(state)
            faces.append(face)
            lefts.append(left_side(face_pieces, row))
            rights.append(right_side(pieces, row))
            sums.append(sum_side(face_pieces))
            back_sums.append(sum_side(pieces))
        waiting, done = [], []
        for n in range(group + ahead):
            if n < group:
                waiting.append(dot(lefts[n], rights[n]))
            if n >= ahead and n - ahead < group:
                k = n - ahead
                high, low = pair_weights(waiting[k], radius + face_radius)
                done.append(
                    (
                        dot(sums[k], jnp.concatenate([high, low], axis=0)),
                        dot(back_sums[k], jnp.concatenate([high, low], axis=1), ((1,), (1,))),
                    )
                )
        for k in range(group):
            onto, back = moment(states[k], done[k][0]), moment(faces[k], done[k][1])
            device, cell = blocks[k]
            for axis in range(3):
                line = time_step * damping * back[axis : axis + 1]
                at = pl.ds(g * group + k, 1)
                if second:
                    line = line + before_ref[axis, at, :]
                react_ref[axis, at, :] = line
                line = part_ref[device, axis, pl.ds(cell, 1), :]
                part_ref[device, axis, pl.ds(cell, 1), :] = line + damping * onto[axis : axis + 1]
        return carry

    lax.fori_loop(0, count // group, several, 0)
    for k in range(nrefs):
        out_ref[pl.ds(starts[k], devices)] = part_ref[pl.ds(k * devices, devices)]


def pack(ct, cc, crosses, track, refs, out_ref):
    gathered = Gathered(refs, crosses, track)
    fields = refs[0].shape[1]
    c_index = lax.axis_index("cross")
    row = jnp.where(track < lax.axis_size("track") - 1, 0, ct - 1)
    for p in range(cc + 2):
        step = -1 if p == 0 else (1 if p == cc + 1 else 0)
        device = jnp.clip(c_index + step, 0, crosses - 1)
        cell = row * cc + (p - 1) % cc
        for f in range(fields):
            out_ref[pl.ds(p * fields + f, 1), :] = gathered.line(0, device, f, cell)


def first_kernel(
    count_from, x_from, v_from, own_ref, live_ref, spread_ref, count_ref, x_ref, v_ref, sems
):
    copies = [
        pltpu.make_async_copy(source, target, sems.at[k])
        for k, (source, target) in enumerate(
            ((count_from, count_ref), (x_from, x_ref), (v_from, v_ref))
        )
    ]
    for copy in copies:
        copy.start()
    for copy in copies:
        copy.wait()
    ct, cc = count_ref.shape
    shape = live_ref.shape
    row = lax.broadcasted_iota(jnp.int32, shape, 0)
    lane = lax.broadcasted_iota(jnp.int32, shape, 1)
    count = jnp.zeros(shape, jnp.int32)
    for cell in range(ct * cc):
        count = jnp.where(row == cell, count_ref[cell // cc, cell % cc], count)
    live = lane < count
    live_ref[...] = jnp.where(live, 1.0, 0.0)
    for axis in range(3):
        x, v = x_ref[axis], v_ref[axis]
        if axis == 0:
            x = jnp.where(live, x, far)
        own_ref[axis] = x
        for k in range(spread_ref.shape[0]):
            spread_ref[k, axis] = x
            spread_ref[k, axis + 3] = v


def update_kernel(second, live_ref, x_ref, v_ref, inner_ref, outer_ref, back_ref, *rest):
    if second:
        react_ref, *outs = rest
        outs[2][...] = react_ref[...]
    else:
        outs = rest
    live = live_ref[...] > 0.5
    for axis in range(3):
        force = jnp.where(live, inner_ref[axis] + outer_ref[axis], 0.0)
        for k in range(back_ref.shape[0]):
            force = force + back_ref[k, axis]
        x, v = advanced(x_ref[axis], v_ref[axis], force, axis)
        outs[0][axis] = x
        outs[1][axis] = v
        if not second:
            outs[2][axis] = jnp.where(live, x, far) if axis == 0 else x
            for k in range(back_ref.shape[0]):
                outs[3][k, axis] = force


def call(kernel, name, there, args, outs, scratch, flops, keep=True):
    specs = [pl.BlockSpec(memory_space=pltpu.HBM)] * len(there)
    specs += [pl.BlockSpec(memory_space=VMEM)] * len(args)
    there = [pltpu.with_memory_space_constraint(a, pltpu.HBM) for a in there]
    args = [pltpu.with_memory_space_constraint(a, VMEM_SPACE) for a in args]
    outs = [s if isinstance(s[0], tuple) else (s, f32) for s in outs]
    shapes = [VMEM(s, t) if keep else jax.ShapeDtypeStruct(s, t) for s, t in outs]
    return pl.pallas_call(
        kernel,
        name=name,
        out_shape=shapes,
        in_specs=specs,
        out_specs=[pl.BlockSpec(memory_space=VMEM)] * len(outs),
        scratch_shapes=scratch,
        compiler_params=pltpu.CompilerParams(vmem_limit_bytes=scratch_bytes),
        cost_estimate=pl.CostEstimate(flops=flops, transcendentals=0, bytes_accessed=0),
    )(*there, *args)


def body(
    particle_offset,
    particle_velocity,
    cell_count,
    face_offset,
    face_velocity,
    face_route,
    face_cell,
):
    _, ct, cc, slots = particle_offset.shape
    cells = ct * cc
    own_faces, _, faces = face_offset.shape
    vehicles, tracks, crosses = [lax.axis_size(a) for a in ("vehicle", "track", "cross")]
    pair = tracks == 2
    nrefs = 2 if pair else 1
    devices = tracks * crosses
    wide = cc + 2
    grid_slots = (ct + 2) * wide
    ring_slots = [
        VMEM((grid_slots * 8, slots), f32),
        VMEM((grid_slots, slots, 80), bf16),
        VMEM((grid_slots, 32, 2 * slots), bf16),
    ]
    right = ((cells, 80, 2 * slots), bf16)
    block = (3, cells, slots)
    swap = [(0, 1), (1, 0)]
    travel = []
    for e in range(vehicles - 1):
        last, following = e * tracks + tracks - 1, (e + 1) * tracks
        travel += [(last, following), (following, last)]

    def exchange(a, axes):
        return lax.all_to_all(a, axes, split_axis=0, concat_axis=0, tiled=True)

    def gather_track(a):
        if pair:
            return [a, lax.ppermute(a, "track", swap)]
        return [lax.all_gather(a, "track", axis=0, tiled=True)]

    x = particle_offset.reshape(block)
    v = particle_velocity.reshape(block)
    offset_rows = jnp.transpose(face_offset, (1, 0, 2))
    velocity_rows = jnp.transpose(face_velocity, (1, 0, 2))
    own, live, spread = call(
        first_kernel,
        "first",
        [cell_count, x, v],
        [],
        [block, (cells, slots), (crosses, 6, cells, slots)],
        [
            SMEM((ct, cc), jnp.int32),
            VMEM(block, f32),
            VMEM(block, f32),
            pltpu.SemaphoreType.DMA((3,)),
        ],
        10**6,
    )
    reaction = everyone = beyond = None
    for substep in range(2):
        second = substep == 1
        mine = exchange(spread, ("track", "cross") if second else "cross")
        inner, rights = call(
            functools.partial(inner_kernel, ct, cc),
            "inner",
            [],
            [own, v],
            [block, right],
            ring_slots,
            10**9,
        )
        mine, inner = lax.optimization_barrier((mine, inner))
        if second:
            extra, before = [mine], [reaction]
        else:
            everyone, extra, before = gather_track(mine), [], []
        part, reaction, packed = call(
            functools.partial(face_kernel, second, ct, cc, crosses, nrefs),
            "faces",
            [face_route.reshape(own_faces), face_cell],
            [offset_rows, velocity_rows] + everyone + extra + before,
            [
                (devices, 3, cells, slots),
                (3, own_faces, faces),
                (wide * (3 if second else 6), slots),
            ],
            [
                VMEM((devices * cells * 8, slots), f32),
                VMEM((own_faces * 8, faces), f32),
                VMEM((devices, 3, cells, slots), f32),
                SMEM((own_faces,), jnp.int32),
                SMEM((own_faces,), jnp.int32),
                pltpu.SemaphoreType.DMA((2,)),
            ],
            4 * 10**9,
        )
        across = lax.ppermute(packed, ("vehicle", "track"), travel)
        if second:
            halo_extra = [across]
        else:
            beyond, halo_extra = across, []
        outer = call(
            functools.partial(outer_kernel, ct, cc, crosses, nrefs, second),
            "outer",
            [],
            [own, v, rights] + everyone + [beyond] + extra + halo_extra,
            [block],
            ring_slots,
            10**9,
        )[0]
        returned, outer = lax.optimization_barrier(
            (exchange(part, ("track", "cross")), outer)
        )
        new = call(
            functools.partial(update_kernel, second),
            "update",
            [],
            [live, x, v, inner, outer, returned] + ([reaction] if second else []),
            [block, block]
            + ([(3, own_faces, faces)] if second else [block, (devices, 3, cells, slots)]),
            [],
            10**6,
            not second,
        )
        x, v = new[:2]
        if second:
            reaction = new[2]
        else:
            own, spread = new[2:]
    shape = particle_offset.shape
    return (x.reshape(shape), v.reshape(shape), jnp.transpose(reaction, (1, 0, 2)))


def solution(mesh):
    in_specs = (
        P(None, ("vehicle", "track"), "cross", None),
        P(None, ("vehicle", "track"), "cross", None),
        P(("vehicle", "track"), "cross"),
        P(("vehicle", "track", "cross"), None, None),
        P(("vehicle", "track", "cross"), None, None),
        P(("vehicle", "track", "cross"), None),
        P(("vehicle", "track", "cross")),
    )
    out_specs = (
        P(None, ("vehicle", "track"), "cross", None),
        P(None, ("vehicle", "track"), "cross", None),
        P(("vehicle", "track", "cross"), None, None),
    )
    return jax.shard_map(body, mesh=mesh, in_specs=in_specs, out_specs=out_specs, check_vma=False)
```

```python
import functools

import jax
import jax.numpy as jnp
from jax import lax
from jax.experimental import pallas as pl
from jax.experimental.pallas import tpu as pltpu
from jax.sharding import PartitionSpec as P

radius = 0.1
face_radius = 0.15
stiffness = 100.0
damping = 40.0
soften = 0.05
time_step = 0.02
gravity = 9.81

far = 1000.0
ahead = 8
columns = 4
faces_at_once = 64
early, late = 2, 4
scratch_bytes = 20 * 2**20
f32 = jnp.float32
bf16 = jnp.bfloat16
falls = (0.0, 0.0, -gravity)
VMEM = pltpu.VMEM
SMEM = pltpu.SMEM
VMEM_SPACE = pltpu.MemorySpace.VMEM


def split3(a):
    high = a.astype(bf16).astype(f32)
    rest = a - high
    mid = rest.astype(bf16).astype(f32)
    return high, mid, rest - mid


def features(state, eps):
    row = lax.broadcasted_iota(jnp.int32, state.shape, 0)
    turned = pltpu.roll(state, 5, 0)
    square = jnp.sum(jnp.where(row < 3, state * state, 0.0), axis=0, keepdims=True) + eps
    cross = jnp.sum(jnp.where(row < 3, state * turned, 0.0), axis=0, keepdims=True)
    full = jnp.where(row == 6, square, jnp.where(row == 7, cross, state))
    return split3(full), row


def left_side(pieces, row):
    p1, p2, p3 = pieces
    ones = jnp.where(row >= 6, 1.0, 0.0)
    zero = jnp.zeros_like(p1)
    stack = jnp.concatenate([p1, p1, p2, p1, p3, p2, ones, ones, ones, zero], axis=0)
    return jnp.transpose(stack).astype(bf16)


def right_side(pieces, row):
    def for_square(p, first):
        return jnp.where(row < 3, -2.0 * p, jnp.where(row == 6, 1.0 if first else 0.0, 0.0))

    def for_closing(p, first):
        swapped = jnp.where(row < 3, pltpu.roll(p, 5, 0), pltpu.roll(p, 3, 0))
        return jnp.where(row < 6, -swapped, jnp.where(row == 7, 1.0 if first else 0.0, 0.0))

    halves = []
    for side, keep in ((for_square, 6), (for_closing, 7)):
        b1, b2, b3 = [side(p, k == 0) for k, p in enumerate(pieces)]
        q = [jnp.where(row == keep, p, 0.0) for p in pieces]
        halves.append(jnp.concatenate([b1, b2, b1, b3, b1, b2] + q + [jnp.zeros_like(b1)], axis=0))
    return jnp.concatenate(halves, axis=1).astype(bf16)


def sum_side(pieces):
    p1, p2, p3 = pieces
    stack = jnp.concatenate([p1, p2, p3, jnp.ones_like(p1)], axis=0).astype(bf16)
    return jnp.concatenate([stack, stack], axis=1)


def pair_weights(product, reach):
    n = product.shape[1] // 2
    square = jnp.maximum(product[:, :n], soften * soften * 0.5)
    inverse = lax.rsqrt(square)
    weight = jnp.maximum(reach * inverse - 1.0, 0.0) * (
        stiffness / damping - product[:, n:] * inverse
    )
    high = weight.astype(bf16)
    low = (weight - high.astype(f32)).astype(bf16)
    return high, low


def dot(a, b, contract=((1,), (0,))):
    return lax.dot_general(a, b, (contract, ((), ())), preferred_element_type=f32)


def moment(state, sums):
    total = sums[0:8] + sums[8:16] + sums[16:24]
    return state * sums[24:25] - total


def advanced(x, v, force, axis):
    v = v + time_step * (force + falls[axis])
    return x + time_step * v, v


def put_own(state_ref, x_ref, v_ref, ct, cc):
    cells = lax.broadcasted_iota(jnp.int32, (cc, 128), 0).astype(f32)
    for r in range(ct):
        base = ((r + 1) * (cc + 2) + 1) * 8
        for axis in range(3):
            x = x_ref[axis, pl.ds(r * cc, cc), :]
            if axis == 0:
                x = x + (r + 1 - (ct + 1) / 2)
            if axis == 1:
                x = x + (cells + (1 - (cc + 1) / 2))
            state_ref[pl.ds(base + axis, cc, stride=8), :] = x
            state_ref[pl.ds(base + 3 + axis, cc, stride=8), :] = v_ref[axis, pl.ds(r * cc, cc), :]


def build_left(state_ref, left_ref, sum_ref, slots):
    for slot in slots:
        pieces, row = features(state_ref[pl.ds(slot * 8, 8), :], 0.0)
        left_ref[slot] = left_side(pieces, row)
        sum_ref[slot] = sum_side(pieces)


def build_right(state_ref, right_ref, slots):
    for k, slot in enumerate(slots):
        pieces, row = features(state_ref[pl.ds(slot * 8, 8), :], soften * soften)
        right_ref[k] = right_side(pieces, row)


def pushes(left_ref, sum_ref, right_ref, jobs):
    todo = [(k, block, slot) for k, (block, others) in enumerate(jobs) for slot in others]
    totals = [None] * len(jobs)
    waiting = []
    for n in range(len(todo) + ahead):
        if n < len(todo):
            k, block, slot = todo[n]
            waiting.append((k, slot, dot(left_ref[slot], right_ref[block])))
        if n >= ahead:
            k, slot, product = waiting.pop(0)
            high, low = pair_weights(product, 2.0 * radius)
            part = dot(sum_ref[slot], jnp.concatenate([high, low], axis=0))
            totals[k] = part if totals[k] is None else totals[k] + part
    return totals


def store_rows(out_ref, values, index, add):
    for axis in range(3):
        line = damping * values[axis : axis + 1]
        if add:
            line = line + out_ref[axis, pl.ds(index, 1), :]
        out_ref[axis, pl.ds(index, 1), :] = line


def inner_kernel(ct, cc, x_ref, v_ref, out_ref, right_ref, state_ref, left_ref, sum_ref):
    wide = cc + 2
    own = [(r + 1) * wide + c + 1 for r in range(ct) for c in range(cc)]
    put_own(state_ref, x_ref, v_ref, ct, cc)
    build_left(state_ref, left_ref, sum_ref, own)
    build_right(state_ref, right_ref, own)

    def finish(cells):
        jobs, places = [], []
        for c, steps in cells:
            for r in range(ct):
                near = range(max(r - 1, 0), min(r + 2, ct))
                jobs.append(
                    (r * cc + c, [(q + 1) * wide + c + 1 + d for q in near for d in steps])
                )
                places.append(((r + 1) * wide + c + 1, r * cc + c))
        for sums, (slot, index) in zip(pushes(left_ref, sum_ref, right_ref, jobs), places):
            start = slot * 8 if isinstance(slot, int) else pl.multiple_of(slot * 8, 8)
            store_rows(out_ref, moment(state_ref[pl.ds(start, 8), :], sums), index, False)

    def several(step, carry):
        finish([(1 + step * columns + k, (-1, 0, 1)) for k in range(columns)])
        return carry

    assert cc >= 2
    middle = cc - 2
    lax.fori_loop(0, middle // columns, several, 0)
    rest = [(c, (-1, 0, 1)) for c in range(1 + middle // columns * columns, cc - 1)]
    finish(rest + [(0, (0, 1)), (cc - 1, (-1, 0))])


class Gathered:
    def __init__(self, refs, crosses, track):
        self.refs, self.crosses, self.track = refs, crosses, track

    def line(self, shift, device, field, cell):
        if len(self.refs) == 2:
            return self.refs[0 if shift == 0 else 1][device, field, pl.ds(cell, 1), :]
        tracks = self.refs[0].shape[0] // self.crosses
        track = jnp.clip(self.track + shift, 0, tracks - 1)
        return self.refs[0][track * self.crosses + device, field, pl.ds(cell, 1), :]


def outer_kernel(ct, cc, crosses, nrefs, second, x_ref, v_ref, right_ref, *rest):
    track, c_index = lax.axis_index("track"), lax.axis_index("cross")
    vehicle = lax.axis_index("vehicle")
    vehicles, tracks = lax.axis_size("vehicle"), lax.axis_size("track")
    gathered = [Gathered(rest[:nrefs], crosses, track)]
    halos = [rest[nrefs]]
    rest = rest[nrefs + 1 :]
    if second:
        gathered.append(Gathered(rest[:1], crosses, track))
        halos.append(rest[1])
        rest = rest[2:]
    out_ref, state_ref, left_ref, sum_ref = rest
    wide = cc + 2
    has_low = c_index > 0
    has_high = c_index < crosses - 1
    put_own(state_ref, x_ref, v_ref, ct, cc)

    def place(slot, rr, p, load, ok):
        for axis in range(3):
            x, v = load(axis, 6, 0), load(axis + 3, 6, 0)
            if second:
                x, v = advanced(x, v, load(axis, 3, 1), axis)
            if axis == 0:
                x = x + (rr - (ct + 1) / 2)
                x = jnp.where(ok, x, far)
            if axis == 1:
                x = jnp.where(ok, x + (p - (cc + 1) / 2), 0.0)
            state_ref[pl.ds(slot * 8 + axis, 1), :] = x
            state_ref[pl.ds(slot * 8 + 3 + axis, 1), :] = jnp.where(ok, v, 0.0)

    def from_all(shift, row, p):
        step = -1 if p == 0 else (1 if p == cc + 1 else 0)
        device = jnp.clip(c_index + step, 0, crosses - 1)
        cell = row * cc + (p - 1) % cc
        return lambda f, n, k: gathered[k].line(shift, device, f, cell)

    def from_halo(p):
        return lambda f, n, k: halos[k][pl.ds(p * n + f, 1), :]

    for rr, shift, row in ((0, -1, ct - 1), (ct + 1, 1, 0)):
        if shift < 0:
            inside, exists = track > 0, (track > 0) | (vehicle > 0)
        else:
            inside = track < tracks - 1
            exists = inside | (vehicle < vehicles - 1)
        for p in range(wide):
            a, b = from_all(shift, row, p), from_halo(p)

            def load(f, n, k, a=a, b=b):
                return jnp.where(inside, a(f, n, k), b(f, n, k))

            ok = exists
            if p == 0:
                ok = jnp.logical_and(ok, has_low)
            if p == cc + 1:
                ok = jnp.logical_and(ok, has_high)
            place(rr * wide + p, rr, p, load, ok)
    for r in range(ct):
        place((r + 1) * wide, r + 1, 0, from_all(0, r, 0), has_low)
        place((r + 1) * wide + cc + 1, r + 1, cc + 1, from_all(0, r, cc + 1), has_high)
    ring = [rr * wide + p for rr in (0, ct + 1) for p in range(wide)]
    ring += [(r + 1) * wide + p for r in range(ct) for p in (0, cc + 1)]
    build_left(state_ref, left_ref, sum_ref, ring)

    def finish(jobs, places, add):
        for sums, (slot, index) in zip(pushes(left_ref, sum_ref, right_ref, jobs), places):
            start = slot * 8 if isinstance(slot, int) else pl.multiple_of(slot * 8, 8)
            store_rows(out_ref, moment(state_ref[pl.ds(start, 8), :], sums), index, add)

    if ct != 2:
        out_ref[...] = jnp.zeros_like(out_ref)

    def several(step, carry):
        jobs, places = [], []
        for k in range(columns):
            c = step * columns + k
            for r, rr in ((0, 0), (ct - 1, ct + 1)):
                jobs.append((r * cc + c, [rr * wide + c + d for d in range(3)]))
                places.append(((r + 1) * wide + c + 1, r * cc + c))
        finish(jobs, places, ct != 2)
        return carry

    lax.fori_loop(0, cc // columns, several, 0)
    jobs, places = [], []
    for r in range(ct):
        near = range(max(r - 1, 0), min(r + 2, ct))
        for c, p in ((0, 0), (cc - 1, cc + 1)):
            jobs.append((r * cc + c, [(q + 1) * wide + p for q in near]))
            places.append(((r + 1) * wide + c + 1, r * cc + c))
    finish(jobs, places, True)


def face_kernel(
    second, ct, cc, crosses, nrefs, route_from, cell_from, offset_ref, velocity_ref, *rest
):
    all_refs, rest = rest[:nrefs], rest[nrefs:]
    if second:
        force_ref, before_ref, *rest = rest
    out_ref, react_ref, halo_ref, state_ref, face_ref, part_ref, route_ref, cell_ref, sems = rest
    copies = [
        pltpu.make_async_copy(route_from, route_ref, sems.at[0]),
        pltpu.make_async_copy(cell_from, cell_ref, sems.at[1]),
    ]
    for copy in copies:
        copy.start()
    devices, _, cells, _ = all_refs[0].shape
    count = offset_ref.shape[1]
    track = lax.axis_index("track")
    pack(ct, cc, crosses, track, [force_ref] if second else all_refs, halo_ref)
    starts = [jnp.bitwise_xor(k, track) * devices if nrefs == 2 else 0 for k in range(nrefs)]
    for k in range(nrefs):

        def spread(device, carry, k=k):
            base = pl.multiple_of((k * devices + device) * cells * 8, 8)
            for axis in range(3):
                x, v = all_refs[k][device, axis], all_refs[k][device, axis + 3]
                if second:
                    x, v = advanced(x, v, force_ref[starts[k] + device, axis], axis)
                state_ref[pl.ds(base + axis, cells, stride=8), :] = x
                state_ref[pl.ds(base + 3 + axis, cells, stride=8), :] = v
                part_ref[k * devices + device, axis] = jnp.zeros_like(x)
            return carry

        lax.fori_loop(0, devices, spread, 0, unroll=min(devices, 4))
    for axis in range(3):
        y, w = offset_ref[axis], velocity_ref[axis]
        if second:
            y = y + time_step * w
        face_ref[pl.ds(axis, count, stride=8), :] = y
        face_ref[pl.ds(3 + axis, count, stride=8), :] = w
    for copy in copies:
        copy.wait()

    def block_of(f):
        target = route_ref[f]
        where, across = lax.div(target, crosses), lax.rem(target, crosses)
        if nrefs == 2:
            where = jnp.bitwise_xor(where, track)
        return where * crosses + across, cell_ref[f]

    group = next(n for n in (faces_at_once, 16, 4, 2, 1) if count % n == 0)

    def several(g, carry):
        blocks, states, rights, back_sums, products, done = {}, {}, {}, {}, {}, {}
        faces, lefts, sums = {}, {}, {}
        for n in range(group + early + ahead + late):
            k = n
            if k < group:
                blocks[k] = block_of(g * group + k)
                place = (blocks[k][0] * cells + blocks[k][1]) * 8
                states[k] = state_ref[pl.ds(pl.multiple_of(place, 8), 8), :]
                pieces, row = features(states[k], soften * soften)
                rights[k], back_sums[k] = right_side(pieces, row), sum_side(pieces)
                faces[k] = face_ref[pl.ds(pl.multiple_of((g * group + k) * 8, 8), 8), :]
                pieces, _ = features(faces[k], 0.0)
                lefts[k], sums[k] = left_side(pieces, row), sum_side(pieces)
            k = n - early
            if 0 <= k < group:
                products[k] = dot(lefts.pop(k), rights.pop(k))
            k = n - early - ahead
            if 0 <= k < group:
                high, low = pair_weights(products.pop(k), radius + face_radius)
                done[k] = (
                    dot(sums.pop(k), jnp.concatenate([high, low], axis=0)),
                    dot(
                        back_sums.pop(k), jnp.concatenate([high, low], axis=1), ((1,), (1,))
                    ),
                )
            k = n - early - ahead - late
            if 0 <= k < group:
                f = g * group + k
                onto, back = done.pop(k)
                onto, back = moment(states.pop(k), onto), moment(faces.pop(k), back)
                device, cell = blocks[k]
                for axis in range(3):
                    line = time_step * damping * back[axis : axis + 1]
                    if second:
                        line = line + before_ref[axis, pl.ds(f, 1), :]
                    react_ref[axis, pl.ds(f, 1), :] = line
                    line = part_ref[device, axis, pl.ds(cell, 1), :]
                    line = line + damping * onto[axis : axis + 1]
                    part_ref[device, axis, pl.ds(cell, 1), :] = line
        return carry

    lax.fori_loop(0, count // group, several, 0)
    for k in range(nrefs):
        out_ref[pl.ds(starts[k], devices)] = part_ref[pl.ds(k * devices, devices)]


def pack(ct, cc, crosses, track, refs, out_ref):
    gathered = Gathered(refs, crosses, track)
    fields = refs[0].shape[1]
    c_index = lax.axis_index("cross")
    row = jnp.where(track < lax.axis_size("track") - 1, 0, ct - 1)
    for p in range(cc + 2):
        step = -1 if p == 0 else (1 if p == cc + 1 else 0)
        device = jnp.clip(c_index + step, 0, crosses - 1)
        cell = row * cc + (p - 1) % cc
        for f in range(fields):
            out_ref[pl.ds(p * fields + f, 1), :] = gathered.line(0, device, f, cell)


def first_kernel(
    count_from, x_from, v_from, own_ref, live_ref, spread_ref, count_ref, x_ref, v_ref, sems
):
    copies = [
        pltpu.make_async_copy(source, target, sems.at[k])
        for k, (source, target) in enumerate(
            ((count_from, count_ref), (x_from, x_ref), (v_from, v_ref))
        )
    ]
    for copy in copies:
        copy.start()
    for copy in copies:
        copy.wait()
    ct, cc = count_ref.shape
    shape = live_ref.shape
    row = lax.broadcasted_iota(jnp.int32, shape, 0)
    lane = lax.broadcasted_iota(jnp.int32, shape, 1)
    count = jnp.zeros(shape, jnp.int32)
    for cell in range(ct * cc):
        count = jnp.where(row == cell, count_ref[cell // cc, cell % cc], count)
    live = lane < count
    live_ref[...] = jnp.where(live, 1.0, 0.0)
    for axis in range(3):
        x, v = x_ref[axis], v_ref[axis]
        if axis == 0:
            x = jnp.where(live, x, far)
        own_ref[axis] = x
        for k in range(spread_ref.shape[0]):
            spread_ref[k, axis] = x
            spread_ref[k, axis + 3] = v


def update_kernel(second, live_ref, x_ref, v_ref, inner_ref, outer_ref, back_ref, *rest):
    if second:
        react_ref, *outs = rest
        outs[2][...] = react_ref[...]
    else:
        outs = rest
    live = live_ref[...] > 0.5
    for axis in range(3):
        force = jnp.where(live, inner_ref[axis] + outer_ref[axis], 0.0)
        for k in range(back_ref.shape[0]):
            force = force + back_ref[k, axis]
        x, v = advanced(x_ref[axis], v_ref[axis], force, axis)
        outs[0][axis] = x
        outs[1][axis] = v
        if not second:
            outs[2][axis] = jnp.where(live, x, far) if axis == 0 else x
            for k in range(back_ref.shape[0]):
                outs[3][k, axis] = force


def call(kernel, name, there, args, outs, scratch, flops, keep=True):
    specs = [pl.BlockSpec(memory_space=pltpu.HBM)] * len(there)
    specs += [pl.BlockSpec(memory_space=VMEM)] * len(args)
    there = [pltpu.with_memory_space_constraint(a, pltpu.HBM) for a in there]
    args = [pltpu.with_memory_space_constraint(a, VMEM_SPACE) for a in args]
    outs = [s if isinstance(s[0], tuple) else (s, f32) for s in outs]
    shapes = [VMEM(s, t) if keep else jax.ShapeDtypeStruct(s, t) for s, t in outs]
    return pl.pallas_call(
        kernel,
        name=name,
        out_shape=shapes,
        in_specs=specs,
        out_specs=[pl.BlockSpec(memory_space=VMEM)] * len(outs),
        scratch_shapes=scratch,
        compiler_params=pltpu.CompilerParams(vmem_limit_bytes=scratch_bytes),
        cost_estimate=pl.CostEstimate(flops=flops, transcendentals=0, bytes_accessed=0),
    )(*there, *args)


def body(
    particle_offset,
    particle_velocity,
    cell_count,
    face_offset,
    face_velocity,
    face_route,
    face_cell,
):
    _, ct, cc, slots = particle_offset.shape
    cells = ct * cc
    own_faces, _, faces = face_offset.shape
    vehicles, tracks, crosses = [lax.axis_size(a) for a in ("vehicle", "track", "cross")]
    pair = tracks == 2
    nrefs = 2 if pair else 1
    devices = tracks * crosses
    wide = cc + 2
    grid_slots = (ct + 2) * wide
    ring_slots = [
        VMEM((grid_slots * 8, slots), f32),
        VMEM((grid_slots, slots, 80), bf16),
        VMEM((grid_slots, 32, 2 * slots), bf16),
    ]
    right = ((cells, 80, 2 * slots), bf16)
    block = (3, cells, slots)
    swap = [(0, 1), (1, 0)]
    travel = []
    for e in range(vehicles - 1):
        last, following = e * tracks + tracks - 1, (e + 1) * tracks
        travel += [(last, following), (following, last)]

    def exchange(a, axes):
        return lax.all_to_all(a, axes, split_axis=0, concat_axis=0, tiled=True)

    def gather_track(a):
        if pair:
            return [a, lax.ppermute(a, "track", swap)]
        return [lax.all_gather(a, "track", axis=0, tiled=True)]

    x = particle_offset.reshape(block)
    v = particle_velocity.reshape(block)
    offset_rows = jnp.transpose(face_offset, (1, 0, 2))
    velocity_rows = jnp.transpose(face_velocity, (1, 0, 2))
    own, live, spread = call(
        first_kernel,
        "first",
        [cell_count, x, v],
        [],
        [block, (cells, slots), (crosses, 6, cells, slots)],
        [
            SMEM((ct, cc), jnp.int32),
            VMEM(block, f32),
            VMEM(block, f32),
            pltpu.SemaphoreType.DMA((3,)),
        ],
        10**6,
    )
    reaction = everyone = beyond = None
    for substep in range(2):
        second = substep == 1
        mine = exchange(spread, ("track", "cross") if second else "cross")
        inner, rights = call(
            functools.partial(inner_kernel, ct, cc),
            "inner",
            [],
            [own, v],
            [block, right],
            ring_slots,
            10**9,
        )
        mine, inner = lax.optimization_barrier((mine, inner))
        if second:
            extra, before = [mine], [reaction]
        else:
            everyone, extra, before = gather_track(mine), [], []
        part, reaction, packed = call(
            functools.partial(face_kernel, second, ct, cc, crosses, nrefs),
            "faces",
            [face_route.reshape(own_faces), face_cell],
            [offset_rows, velocity_rows] + everyone + extra + before,
            [
                (devices, 3, cells, slots),
                (3, own_faces, faces),
                (wide * (3 if second else 6), slots),
            ],
            [
                VMEM((devices * cells * 8, slots), f32),
                VMEM((own_faces * 8, faces), f32),
                VMEM((devices, 3, cells, slots), f32),
                SMEM((own_faces,), jnp.int32),
                SMEM((own_faces,), jnp.int32),
                pltpu.SemaphoreType.DMA((2,)),
            ],
            4 * 10**9,
        )
        across = lax.ppermute(packed, ("vehicle", "track"), travel)
        if second:
            halo_extra = [across]
        else:
            beyond, halo_extra = across, []
        outer = call(
            functools.partial(outer_kernel, ct, cc, crosses, nrefs, second),
            "outer",
            [],
            [own, v, rights] + everyone + [beyond] + extra + halo_extra,
            [block],
            ring_slots,
            10**9,
        )[0]
        returned, outer = lax.optimization_barrier(
            (exchange(part, ("track", "cross")), outer)
        )
        new = call(
            functools.partial(update_kernel, second),
            "update",
            [],
            [live, x, v, inner, outer, returned] + ([reaction] if second else []),
            [block, block]
            + ([(3, own_faces, faces)] if second else [block, (devices, 3, cells, slots)]),
            [],
            10**6,
            not second,
        )
        x, v = new[:2]
        if second:
            reaction = new[2]
        else:
            own, spread = new[2:]
    shape = particle_offset.shape
    return (x.reshape(shape), v.reshape(shape), jnp.transpose(reaction, (1, 0, 2)))


def solution(mesh):
    in_specs = (
        P(None, ("vehicle", "track"), "cross", None),
        P(None, ("vehicle", "track"), "cross", None),
        P(("vehicle", "track"), "cross"),
        P(("vehicle", "track", "cross"), None, None),
        P(("vehicle", "track", "cross"), None, None),
        P(("vehicle", "track", "cross"), None),
        P(("vehicle", "track", "cross")),
    )
    out_specs = (
        P(None, ("vehicle", "track"), "cross", None),
        P(None, ("vehicle", "track"), "cross", None),
        P(("vehicle", "track", "cross"), None, None),
    )
    return jax.shard_map(body, mesh=mesh, in_specs=in_specs, out_specs=out_specs, check_vma=False)
```

```python
import functools

import jax
import jax.numpy as jnp
from jax import lax
from jax.experimental import pallas as pl
from jax.experimental.pallas import tpu as pltpu
from jax.sharding import PartitionSpec as P

radius = 0.1
face_radius = 0.15
stiffness = 100.0
damping = 40.0
soften = 0.05
time_step = 0.02
gravity = 9.81

far = 1000.0
ahead = 8
columns = 4
faces_at_once = 64
early, late = 2, 4
scratch_bytes = 20 * 2**20
f32 = jnp.float32
bf16 = jnp.bfloat16
falls = (0.0, 0.0, -gravity)
VMEM = pltpu.VMEM
SMEM = pltpu.SMEM
VMEM_SPACE = pltpu.MemorySpace.VMEM


def split3(a):
    high = a.astype(bf16).astype(f32)
    rest = a - high
    mid = rest.astype(bf16).astype(f32)
    return high, mid, rest - mid


def features(state, eps):
    row = lax.broadcasted_iota(jnp.int32, state.shape, 0)
    turned = pltpu.roll(state, 5, 0)
    square = jnp.sum(jnp.where(row < 3, state * state, 0.0), axis=0, keepdims=True) + eps
    cross = jnp.sum(jnp.where(row < 3, state * turned, 0.0), axis=0, keepdims=True)
    full = jnp.where(row == 6, square, jnp.where(row == 7, cross, state))
    return split3(full), row


def left_side(pieces, row):
    p1, p2, p3 = pieces
    ones = jnp.where(row >= 6, 1.0, 0.0)
    zero = jnp.zeros_like(p1)
    stack = jnp.concatenate([p1, p1, p2, p1, p3, p2, ones, ones, ones, zero], axis=0)
    return jnp.transpose(stack).astype(bf16)


def right_side(pieces, row):
    def for_square(p, first):
        return jnp.where(row < 3, -2.0 * p, jnp.where(row == 6, 1.0 if first else 0.0, 0.0))

    def for_closing(p, first):
        swapped = jnp.where(row < 3, pltpu.roll(p, 5, 0), pltpu.roll(p, 3, 0))
        return jnp.where(row < 6, -swapped, jnp.where(row == 7, 1.0 if first else 0.0, 0.0))

    halves = []
    for side, keep in ((for_square, 6), (for_closing, 7)):
        b1, b2, b3 = [side(p, k == 0) for k, p in enumerate(pieces)]
        q = [jnp.where(row == keep, p, 0.0) for p in pieces]
        halves.append(jnp.concatenate([b1, b2, b1, b3, b1, b2] + q + [jnp.zeros_like(b1)], axis=0))
    return jnp.concatenate(halves, axis=1).astype(bf16)


def sum_side(pieces):
    p1, p2, p3 = pieces
    stack = jnp.concatenate([p1, p2, p3, jnp.ones_like(p1)], axis=0).astype(bf16)
    return jnp.concatenate([stack, stack], axis=1)


def pair_weights(product, reach):
    n = product.shape[1] // 2
    square = jnp.maximum(product[:, :n], soften * soften * 0.5)
    inverse = lax.rsqrt(square)
    weight = jnp.maximum(reach * inverse - 1.0, 0.0) * (
        stiffness / damping - product[:, n:] * inverse
    )
    high = weight.astype(bf16)
    low = (weight - high.astype(f32)).astype(bf16)
    return high, low


def dot(a, b, contract=((1,), (0,))):
    return lax.dot_general(a, b, (contract, ((), ())), preferred_element_type=f32)


def moment(state, sums):
    total = sums[0:8] + sums[8:16] + sums[16:24]
    return state * sums[24:25] - total


def advanced(x, v, force, axis):
    v = v + time_step * (force + falls[axis])
    return x + time_step * v, v


def put_own(state_ref, x_ref, v_ref, ct, cc):
    cells = lax.broadcasted_iota(jnp.int32, (cc, 128), 0).astype(f32)
    for r in range(ct):
        base = ((r + 1) * (cc + 2) + 1) * 8
        for axis in range(3):
            x = x_ref[axis, pl.ds(r * cc, cc), :]
            if axis == 0:
                x = x + (r + 1 - (ct + 1) / 2)
            if axis == 1:
                x = x + (cells + (1 - (cc + 1) / 2))
            state_ref[pl.ds(base + axis, cc, stride=8), :] = x
            state_ref[pl.ds(base + 3 + axis, cc, stride=8), :] = v_ref[axis, pl.ds(r * cc, cc), :]


def build_left(state_ref, left_ref, sum_ref, slots):
    for slot in slots:
        pieces, row = features(state_ref[pl.ds(slot * 8, 8), :], 0.0)
        left_ref[slot] = left_side(pieces, row)
        sum_ref[slot] = sum_side(pieces)


def build_right(state_ref, right_ref, slots):
    for k, slot in enumerate(slots):
        pieces, row = features(state_ref[pl.ds(slot * 8, 8), :], soften * soften)
        right_ref[k] = right_side(pieces, row)


def pushes(left_ref, sum_ref, right_ref, jobs):
    todo = [(k, block, slot) for k, (block, others) in enumerate(jobs) for slot in others]
    totals = [None] * len(jobs)
    waiting = []
    for n in range(len(todo) + ahead):
        if n < len(todo):
            k, block, slot = todo[n]
            waiting.append((k, slot, dot(left_ref[slot], right_ref[block])))
        if n >= ahead:
            k, slot, product = waiting.pop(0)
            high, low = pair_weights(product, 2.0 * radius)
            part = dot(sum_ref[slot], jnp.concatenate([high, low], axis=0))
            totals[k] = part if totals[k] is None else totals[k] + part
    return totals


def store_rows(out_ref, values, index, add):
    for axis in range(3):
        line = damping * values[axis : axis + 1]
        if add:
            line = line + out_ref[axis, pl.ds(index, 1), :]
        out_ref[axis, pl.ds(index, 1), :] = line


def inner_kernel(ct, cc, x_ref, v_ref, out_ref, right_ref, state_ref, left_ref, sum_ref):
    wide = cc + 2
    own = [(r + 1) * wide + c + 1 for r in range(ct) for c in range(cc)]
    put_own(state_ref, x_ref, v_ref, ct, cc)
    build_left(state_ref, left_ref, sum_ref, own)
    build_right(state_ref, right_ref, own)

    def finish(cells):
        jobs, places = [], []
        for c, steps in cells:
            for r in range(ct):
                near = range(max(r - 1, 0), min(r + 2, ct))
                jobs.append(
                    (r * cc + c, [(q + 1) * wide + c + 1 + d for q in near for d in steps])
                )
                places.append(((r + 1) * wide + c + 1, r * cc + c))
        for sums, (slot, index) in zip(pushes(left_ref, sum_ref, right_ref, jobs), places):
            start = slot * 8 if isinstance(slot, int) else pl.multiple_of(slot * 8, 8)
            store_rows(out_ref, moment(state_ref[pl.ds(start, 8), :], sums), index, False)

    def several(step, carry):
        finish([(1 + step * columns + k, (-1, 0, 1)) for k in range(columns)])
        return carry

    assert cc >= 2
    middle = cc - 2
    lax.fori_loop(0, middle // columns, several, 0)
    rest = [(c, (-1, 0, 1)) for c in range(1 + middle // columns * columns, cc - 1)]
    finish(rest + [(0, (0, 1)), (cc - 1, (-1, 0))])


class Gathered:
    def __init__(self, refs, crosses, track):
        self.refs, self.crosses, self.track = refs, crosses, track

    def line(self, shift, device, field, cell):
        if len(self.refs) == 2:
            return self.refs[0 if shift == 0 else 1][device, field, pl.ds(cell, 1), :]
        tracks = self.refs[0].shape[0] // self.crosses
        track = jnp.clip(self.track + shift, 0, tracks - 1)
        return self.refs[0][track * self.crosses + device, field, pl.ds(cell, 1), :]


def outer_kernel(ct, cc, crosses, nrefs, second, x_ref, v_ref, right_ref, *rest):
    track, c_index = lax.axis_index("track"), lax.axis_index("cross")
    vehicle = lax.axis_index("vehicle")
    vehicles, tracks = lax.axis_size("vehicle"), lax.axis_size("track")
    gathered = [Gathered(rest[:nrefs], crosses, track)]
    halos = [rest[nrefs]]
    rest = rest[nrefs + 1 :]
    if second:
        gathered.append(Gathered(rest[:1], crosses, track))
        halos.append(rest[1])
        rest = rest[2:]
    out_ref, state_ref, left_ref, sum_ref = rest
    wide = cc + 2
    has_low = c_index > 0
    has_high = c_index < crosses - 1
    put_own(state_ref, x_ref, v_ref, ct, cc)

    def place(slot, rr, p, load, ok):
        for axis in range(3):
            x, v = load(axis, 6, 0), load(axis + 3, 6, 0)
            if second:
                x, v = advanced(x, v, load(axis, 3, 1), axis)
            if axis == 0:
                x = x + (rr - (ct + 1) / 2)
                x = jnp.where(ok, x, far)
            if axis == 1:
                x = jnp.where(ok, x + (p - (cc + 1) / 2), 0.0)
            state_ref[pl.ds(slot * 8 + axis, 1), :] = x
            state_ref[pl.ds(slot * 8 + 3 + axis, 1), :] = jnp.where(ok, v, 0.0)

    def from_all(shift, row, p):
        step = -1 if p == 0 else (1 if p == cc + 1 else 0)
        device = jnp.clip(c_index + step, 0, crosses - 1)
        cell = row * cc + (p - 1) % cc
        return lambda f, n, k: gathered[k].line(shift, device, f, cell)

    def from_halo(p):
        return lambda f, n, k: halos[k][pl.ds(p * n + f, 1), :]

    for rr, shift, row in ((0, -1, ct - 1), (ct + 1, 1, 0)):
        if shift < 0:
            inside, exists = track > 0, (track > 0) | (vehicle > 0)
        else:
            inside = track < tracks - 1
            exists = inside | (vehicle < vehicles - 1)
        for p in range(wide):
            a, b = from_all(shift, row, p), from_halo(p)

            def load(f, n, k, a=a, b=b):
                return jnp.where(inside, a(f, n, k), b(f, n, k))

            ok = exists
            if p == 0:
                ok = jnp.logical_and(ok, has_low)
            if p == cc + 1:
                ok = jnp.logical_and(ok, has_high)
            place(rr * wide + p, rr, p, load, ok)
    for r in range(ct):
        place((r + 1) * wide, r + 1, 0, from_all(0, r, 0), has_low)
        place((r + 1) * wide + cc + 1, r + 1, cc + 1, from_all(0, r, cc + 1), has_high)
    ring = [rr * wide + p for rr in (0, ct + 1) for p in range(wide)]
    ring += [(r + 1) * wide + p for r in range(ct) for p in (0, cc + 1)]
    build_left(state_ref, left_ref, sum_ref, ring)

    jobs = []
    for c in range(cc):
        for r in range(ct):
            near = range(max(r - 1, 0), min(r + 2, ct))
            others = [(q + 1) * wide for q in near] if c == 0 else []
            others += [(q + 1) * wide + cc + 1 for q in near] if c == cc - 1 else []
            others += [c + d for d in range(3)] if r == 0 else []
            others += [(ct + 1) * wide + c + d for d in range(3)] if r == ct - 1 else []
            if others:
                jobs.append((r * cc + c, others))
    if ct > 2:
        out_ref[...] = jnp.zeros_like(out_ref)
    for (index, _), sums in zip(jobs, pushes(left_ref, sum_ref, right_ref, jobs)):
        start = ((index // cc + 1) * wide + index % cc + 1) * 8
        store_rows(out_ref, moment(state_ref[pl.ds(start, 8), :], sums), index, False)


def face_kernel(
    second, ct, cc, crosses, nrefs, route_from, cell_from, offset_ref, velocity_ref, *rest
):
    all_refs, rest = rest[:nrefs], rest[nrefs:]
    if second:
        force_ref, before_ref, *rest = rest
    out_ref, react_ref, halo_ref, state_ref, face_ref, part_ref, route_ref, cell_ref, sems = rest
    copies = [
        pltpu.make_async_copy(route_from, route_ref, sems.at[0]),
        pltpu.make_async_copy(cell_from, cell_ref, sems.at[1]),
    ]
    for copy in copies:
        copy.start()
    devices, _, cells, _ = all_refs[0].shape
    count = offset_ref.shape[1]
    track = lax.axis_index("track")
    pack(ct, cc, crosses, track, [force_ref] if second else all_refs, halo_ref)
    starts = [jnp.bitwise_xor(k, track) * devices if nrefs == 2 else 0 for k in range(nrefs)]
    for k in range(nrefs):

        def spread(device, carry, k=k):
            base = pl.multiple_of((k * devices + device) * cells * 8, 8)
            for axis in range(3):
                x, v = all_refs[k][device, axis], all_refs[k][device, axis + 3]
                if second:
                    x, v = advanced(x, v, force_ref[starts[k] + device, axis], axis)
                state_ref[pl.ds(base + axis, cells, stride=8), :] = x
                state_ref[pl.ds(base + 3 + axis, cells, stride=8), :] = v
                part_ref[k * devices + device, axis] = jnp.zeros_like(x)
            return carry

        lax.fori_loop(0, devices, spread, 0, unroll=min(devices, 4))
    for axis in range(3):
        y, w = offset_ref[axis], velocity_ref[axis]
        if second:
            y = y + time_step * w
        face_ref[pl.ds(axis, count, stride=8), :] = y
        face_ref[pl.ds(3 + axis, count, stride=8), :] = w
    for copy in copies:
        copy.wait()

    def block_of(f):
        target = route_ref[f]
        where, across = lax.div(target, crosses), lax.rem(target, crosses)
        if nrefs == 2:
            where = jnp.bitwise_xor(where, track)
        return where * crosses + across, cell_ref[f]

    group = next(n for n in (faces_at_once, 16, 4, 2, 1) if count % n == 0)

    def several(g, carry):
        blocks, states, rights, back_sums, products, done = {}, {}, {}, {}, {}, {}
        faces, lefts, sums = {}, {}, {}
        for n in range(group + early + ahead + late):
            k = n
            if k < group:
                blocks[k] = block_of(g * group + k)
                place = (blocks[k][0] * cells + blocks[k][1]) * 8
                states[k] = state_ref[pl.ds(pl.multiple_of(place, 8), 8), :]
                pieces, row = features(states[k], soften * soften)
                rights[k], back_sums[k] = right_side(pieces, row), sum_side(pieces)
                faces[k] = face_ref[pl.ds(pl.multiple_of((g * group + k) * 8, 8), 8), :]
                pieces, _ = features(faces[k], 0.0)
                lefts[k], sums[k] = left_side(pieces, row), sum_side(pieces)
            k = n - early
            if 0 <= k < group:
                products[k] = dot(lefts.pop(k), rights.pop(k))
            k = n - early - ahead
            if 0 <= k < group:
                high, low = pair_weights(products.pop(k), radius + face_radius)
                done[k] = (
                    dot(sums.pop(k), jnp.concatenate([high, low], axis=0)),
                    dot(
                        back_sums.pop(k), jnp.concatenate([high, low], axis=1), ((1,), (1,))
                    ),
                )
            k = n - early - ahead - late
            if 0 <= k < group:
                f = g * group + k
                onto, back = done.pop(k)
                onto, back = moment(states.pop(k), onto), moment(faces.pop(k), back)
                device, cell = blocks[k]
                for axis in range(3):
                    line = time_step * damping * back[axis : axis + 1]
                    if second:
                        line = line + before_ref[axis, pl.ds(f, 1), :]
                    react_ref[axis, pl.ds(f, 1), :] = line
                    line = part_ref[device, axis, pl.ds(cell, 1), :]
                    line = line + damping * onto[axis : axis + 1]
                    part_ref[device, axis, pl.ds(cell, 1), :] = line
        return carry

    lax.fori_loop(0, count // group, several, 0)
    for k in range(nrefs):
        out_ref[pl.ds(starts[k], devices)] = part_ref[pl.ds(k * devices, devices)]


def pack(ct, cc, crosses, track, refs, out_ref):
    gathered = Gathered(refs, crosses, track)
    fields = refs[0].shape[1]
    c_index = lax.axis_index("cross")
    row = jnp.where(track < lax.axis_size("track") - 1, 0, ct - 1)
    for p in range(cc + 2):
        step = -1 if p == 0 else (1 if p == cc + 1 else 0)
        device = jnp.clip(c_index + step, 0, crosses - 1)
        cell = row * cc + (p - 1) % cc
        for f in range(fields):
            out_ref[pl.ds(p * fields + f, 1), :] = gathered.line(0, device, f, cell)


def first_kernel(
    count_from, x_from, v_from, own_ref, live_ref, spread_ref, count_ref, x_ref, v_ref, sems
):
    copies = [
        pltpu.make_async_copy(source, target, sems.at[k])
        for k, (source, target) in enumerate(
            ((count_from, count_ref), (x_from, x_ref), (v_from, v_ref))
        )
    ]
    for copy in copies:
        copy.start()
    for copy in copies:
        copy.wait()
    ct, cc = count_ref.shape
    shape = live_ref.shape
    row = lax.broadcasted_iota(jnp.int32, shape, 0)
    lane = lax.broadcasted_iota(jnp.int32, shape, 1)
    count = jnp.zeros(shape, jnp.int32)
    for cell in range(ct * cc):
        count = jnp.where(row == cell, count_ref[cell // cc, cell % cc], count)
    live = lane < count
    live_ref[...] = jnp.where(live, 1.0, 0.0)
    for axis in range(3):
        x, v = x_ref[axis], v_ref[axis]
        if axis == 0:
            x = jnp.where(live, x, far)
        own_ref[axis] = x
        for k in range(spread_ref.shape[0]):
            spread_ref[k, axis] = x
            spread_ref[k, axis + 3] = v


def update_kernel(second, live_ref, x_ref, v_ref, inner_ref, outer_ref, back_ref, *rest):
    if second:
        react_ref, *outs = rest
        outs[2][...] = react_ref[...]
    else:
        outs = rest
    live = live_ref[...] > 0.5
    for axis in range(3):
        force = jnp.where(live, inner_ref[axis] + outer_ref[axis], 0.0)
        for k in range(back_ref.shape[0]):
            force = force + back_ref[k, axis]
        x, v = advanced(x_ref[axis], v_ref[axis], force, axis)
        outs[0][axis] = x
        outs[1][axis] = v
        if not second:
            outs[2][axis] = jnp.where(live, x, far) if axis == 0 else x
            for k in range(back_ref.shape[0]):
                outs[3][k, axis] = force


def call(kernel, name, there, args, outs, scratch, flops, keep=True):
    specs = [pl.BlockSpec(memory_space=pltpu.HBM)] * len(there)
    specs += [pl.BlockSpec(memory_space=VMEM)] * len(args)
    there = [pltpu.with_memory_space_constraint(a, pltpu.HBM) for a in there]
    args = [pltpu.with_memory_space_constraint(a, VMEM_SPACE) for a in args]
    outs = [s if isinstance(s[0], tuple) else (s, f32) for s in outs]
    shapes = [VMEM(s, t) if keep else jax.ShapeDtypeStruct(s, t) for s, t in outs]
    return pl.pallas_call(
        kernel,
        name=name,
        out_shape=shapes,
        in_specs=specs,
        out_specs=[pl.BlockSpec(memory_space=VMEM)] * len(outs),
        scratch_shapes=scratch,
        compiler_params=pltpu.CompilerParams(vmem_limit_bytes=scratch_bytes),
        cost_estimate=pl.CostEstimate(flops=flops, transcendentals=0, bytes_accessed=0),
    )(*there, *args)


def body(
    particle_offset,
    particle_velocity,
    cell_count,
    face_offset,
    face_velocity,
    face_route,
    face_cell,
):
    _, ct, cc, slots = particle_offset.shape
    cells = ct * cc
    own_faces, _, faces = face_offset.shape
    vehicles, tracks, crosses = [lax.axis_size(a) for a in ("vehicle", "track", "cross")]
    pair = tracks == 2
    nrefs = 2 if pair else 1
    devices = tracks * crosses
    wide = cc + 2
    grid_slots = (ct + 2) * wide
    ring_slots = [
        VMEM((grid_slots * 8, slots), f32),
        VMEM((grid_slots, slots, 80), bf16),
        VMEM((grid_slots, 32, 2 * slots), bf16),
    ]
    right = ((cells, 80, 2 * slots), bf16)
    block = (3, cells, slots)
    swap = [(0, 1), (1, 0)]
    travel = []
    for e in range(vehicles - 1):
        last, following = e * tracks + tracks - 1, (e + 1) * tracks
        travel += [(last, following), (following, last)]

    def exchange(a, axes):
        return lax.all_to_all(a, axes, split_axis=0, concat_axis=0, tiled=True)

    def gather_track(a):
        if pair:
            return [a, lax.ppermute(a, "track", swap)]
        return [lax.all_gather(a, "track", axis=0, tiled=True)]

    x = particle_offset.reshape(block)
    v = particle_velocity.reshape(block)
    offset_rows = jnp.transpose(face_offset, (1, 0, 2))
    velocity_rows = jnp.transpose(face_velocity, (1, 0, 2))
    own, live, spread = call(
        first_kernel,
        "first",
        [cell_count, x, v],
        [],
        [block, (cells, slots), (crosses, 6, cells, slots)],
        [
            SMEM((ct, cc), jnp.int32),
            VMEM(block, f32),
            VMEM(block, f32),
            pltpu.SemaphoreType.DMA((3,)),
        ],
        10**6,
    )
    reaction = everyone = beyond = None
    for substep in range(2):
        second = substep == 1
        mine = exchange(spread, ("track", "cross") if second else "cross")
        inner, rights = call(
            functools.partial(inner_kernel, ct, cc),
            "inner",
            [],
            [own, v],
            [block, right],
            ring_slots,
            10**9,
        )
        mine, inner = lax.optimization_barrier((mine, inner))
        if second:
            extra, before = [mine], [reaction]
        else:
            everyone, extra, before = gather_track(mine), [], []
        part, reaction, packed = call(
            functools.partial(face_kernel, second, ct, cc, crosses, nrefs),
            "faces",
            [face_route.reshape(own_faces), face_cell],
            [offset_rows, velocity_rows] + everyone + extra + before,
            [
                (devices, 3, cells, slots),
                (3, own_faces, faces),
                (wide * (3 if second else 6), slots),
            ],
            [
                VMEM((devices * cells * 8, slots), f32),
                VMEM((own_faces * 8, faces), f32),
                VMEM((devices, 3, cells, slots), f32),
                SMEM((own_faces,), jnp.int32),
                SMEM((own_faces,), jnp.int32),
                pltpu.SemaphoreType.DMA((2,)),
            ],
            4 * 10**9,
        )
        across = lax.ppermute(packed, ("vehicle", "track"), travel)
        if second:
            halo_extra = [across]
        else:
            beyond, halo_extra = across, []
        outer = call(
            functools.partial(outer_kernel, ct, cc, crosses, nrefs, second),
            "outer",
            [],
            [own, v, rights] + everyone + [beyond] + extra + halo_extra,
            [block],
            ring_slots,
            10**9,
        )[0]
        returned, outer = lax.optimization_barrier(
            (exchange(part, ("track", "cross")), outer)
        )
        new = call(
            functools.partial(update_kernel, second),
            "update",
            [],
            [live, x, v, inner, outer, returned] + ([reaction] if second else []),
            [block, block]
            + ([(3, own_faces, faces)] if second else [block, (devices, 3, cells, slots)]),
            [],
            10**6,
            not second,
        )
        x, v = new[:2]
        if second:
            reaction = new[2]
        else:
            own, spread = new[2:]
    shape = particle_offset.shape
    return (x.reshape(shape), v.reshape(shape), jnp.transpose(reaction, (1, 0, 2)))


def solution(mesh):
    in_specs = (
        P(None, ("vehicle", "track"), "cross", None),
        P(None, ("vehicle", "track"), "cross", None),
        P(("vehicle", "track"), "cross"),
        P(("vehicle", "track", "cross"), None, None),
        P(("vehicle", "track", "cross"), None, None),
        P(("vehicle", "track", "cross"), None),
        P(("vehicle", "track", "cross")),
    )
    out_specs = (
        P(None, ("vehicle", "track"), "cross", None),
        P(None, ("vehicle", "track"), "cross", None),
        P(("vehicle", "track", "cross"), None, None),
    )
    return jax.shard_map(body, mesh=mesh, in_specs=in_specs, out_specs=out_specs, check_vma=False)
```

```python
import functools

import jax
import jax.numpy as jnp
from jax import lax
from jax.experimental import pallas as pl
from jax.experimental.pallas import tpu as pltpu
from jax.sharding import PartitionSpec as P

radius = 0.1
face_radius = 0.15
stiffness = 100.0
damping = 40.0
soften = 0.05
time_step = 0.02
gravity = 9.81

far = 1000.0
ahead = 8
columns = 4
faces_at_once = 64
early, late = 2, 4
scratch_bytes = 20 * 2**20
f32 = jnp.float32
bf16 = jnp.bfloat16
falls = (0.0, 0.0, -gravity)
VMEM = pltpu.VMEM
SMEM = pltpu.SMEM
VMEM_SPACE = pltpu.MemorySpace.VMEM


def split3(a):
    high = a.astype(bf16).astype(f32)
    rest = a - high
    mid = rest.astype(bf16).astype(f32)
    return high, mid, rest - mid


def features(state, eps):
    row = lax.broadcasted_iota(jnp.int32, state.shape, 0)
    turned = pltpu.roll(state, 5, 0)
    square = jnp.sum(jnp.where(row < 3, state * state, 0.0), axis=0, keepdims=True) + eps
    cross = jnp.sum(jnp.where(row < 3, state * turned, 0.0), axis=0, keepdims=True)
    full = jnp.where(row == 6, square, jnp.where(row == 7, cross, state))
    return split3(full), row


def left_side(pieces, row):
    p1, p2, p3 = pieces
    ones = jnp.where(row >= 6, 1.0, 0.0)
    zero = jnp.zeros_like(p1)
    stack = jnp.concatenate([p1, p1, p2, p1, p3, p2, ones, ones, ones, zero], axis=0)
    return jnp.transpose(stack).astype(bf16)


def right_side(pieces, row):
    def for_square(p, first):
        return jnp.where(row < 3, -2.0 * p, jnp.where(row == 6, 1.0 if first else 0.0, 0.0))

    def for_closing(p, first):
        swapped = jnp.where(row < 3, pltpu.roll(p, 5, 0), pltpu.roll(p, 3, 0))
        return jnp.where(row < 6, -swapped, jnp.where(row == 7, 1.0 if first else 0.0, 0.0))

    halves = []
    for side, keep in ((for_square, 6), (for_closing, 7)):
        b1, b2, b3 = [side(p, k == 0) for k, p in enumerate(pieces)]
        q = [jnp.where(row == keep, p, 0.0) for p in pieces]
        halves.append(jnp.concatenate([b1, b2, b1, b3, b1, b2] + q + [jnp.zeros_like(b1)], axis=0))
    return jnp.concatenate(halves, axis=1).astype(bf16)


def sum_side(pieces):
    p1, p2, p3 = pieces
    stack = jnp.concatenate([p1, p2, p3, jnp.ones_like(p1)], axis=0).astype(bf16)
    return jnp.concatenate([stack, stack], axis=1)


def pair_weights(product, reach):
    n = product.shape[1] // 2
    square = jnp.maximum(product[:, :n], soften * soften * 0.5)
    inverse = lax.rsqrt(square)
    weight = jnp.maximum(reach * inverse - 1.0, 0.0) * (
        stiffness / damping - product[:, n:] * inverse
    )
    high = weight.astype(bf16)
    low = (weight - high.astype(f32)).astype(bf16)
    return high, low


def dot(a, b, contract=((1,), (0,))):
    return lax.dot_general(a, b, (contract, ((), ())), preferred_element_type=f32)


def moment(state, sums):
    total = sums[0:8] + sums[8:16] + sums[16:24]
    return state * sums[24:25] - total


def advanced(x, v, force, axis):
    v = v + time_step * (force + falls[axis])
    return x + time_step * v, v


def put_own(state_ref, x_ref, v_ref, ct, cc):
    cells = lax.broadcasted_iota(jnp.int32, (cc, 128), 0).astype(f32)
    for r in range(ct):
        base = ((r + 1) * (cc + 2) + 1) * 8
        for axis in range(3):
            x = x_ref[axis, pl.ds(r * cc, cc), :]
            if axis == 0:
                x = x + (r + 1 - (ct + 1) / 2)
            if axis == 1:
                x = x + (cells + (1 - (cc + 1) / 2))
            state_ref[pl.ds(base + axis, cc, stride=8), :] = x
            state_ref[pl.ds(base + 3 + axis, cc, stride=8), :] = v_ref[axis, pl.ds(r * cc, cc), :]


def build_left(state_ref, left_ref, sum_ref, slots):
    for slot in slots:
        pieces, row = features(state_ref[pl.ds(slot * 8, 8), :], 0.0)
        left_ref[slot] = left_side(pieces, row)
        sum_ref[slot] = sum_side(pieces)


def build_right(state_ref, right_ref, slots):
    for k, slot in enumerate(slots):
        pieces, row = features(state_ref[pl.ds(slot * 8, 8), :], soften * soften)
        right_ref[k] = right_side(pieces, row)


def pushes(left_ref, sum_ref, right_ref, jobs):
    todo = [(k, block, slot) for k, (block, others) in enumerate(jobs) for slot in others]
    totals = [None] * len(jobs)
    waiting = []
    for n in range(len(todo) + ahead):
        if n < len(todo):
            k, block, slot = todo[n]
            waiting.append((k, slot, dot(left_ref[slot], right_ref[block])))
        if n >= ahead:
            k, slot, product = waiting.pop(0)
            high, low = pair_weights(product, 2.0 * radius)
            part = dot(sum_ref[slot], jnp.concatenate([high, low], axis=0))
            totals[k] = part if totals[k] is None else totals[k] + part
    return totals


def store_rows(out_ref, values, index, add):
    for axis in range(3):
        line = damping * values[axis : axis + 1]
        if add:
            line = line + out_ref[axis, pl.ds(index, 1), :]
        out_ref[axis, pl.ds(index, 1), :] = line


def inner_kernel(ct, cc, x_ref, v_ref, out_ref, right_ref, state_ref, left_ref, sum_ref):
    wide = cc + 2
    own = [(r + 1) * wide + c + 1 for r in range(ct) for c in range(cc)]
    put_own(state_ref, x_ref, v_ref, ct, cc)
    build_left(state_ref, left_ref, sum_ref, own)
    build_right(state_ref, right_ref, own)

    def finish(cells):
        jobs, places = [], []
        for c, steps in cells:
            for r in range(ct):
                near = range(max(r - 1, 0), min(r + 2, ct))
                jobs.append(
                    (r * cc + c, [(q + 1) * wide + c + 1 + d for q in near for d in steps])
                )
                places.append(((r + 1) * wide + c + 1, r * cc + c))
        for sums, (slot, index) in zip(pushes(left_ref, sum_ref, right_ref, jobs), places):
            start = slot * 8 if isinstance(slot, int) else pl.multiple_of(slot * 8, 8)
            store_rows(out_ref, moment(state_ref[pl.ds(start, 8), :], sums), index, False)

    def several(step, carry):
        finish([(1 + step * columns + k, (-1, 0, 1)) for k in range(columns)])
        return carry

    assert cc >= 2
    middle = cc - 2
    lax.fori_loop(0, middle // columns, several, 0)
    rest = [(c, (-1, 0, 1)) for c in range(1 + middle // columns * columns, cc - 1)]
    finish(rest + [(0, (0, 1)), (cc - 1, (-1, 0))])


class Gathered:
    def __init__(self, refs, crosses, track):
        self.refs, self.crosses, self.track = refs, crosses, track

    def line(self, shift, device, field, cell):
        if len(self.refs) == 2:
            own = isinstance(shift, int) and shift == 0
            return self.refs[0 if own else 1][device, field, pl.ds(cell, 1), :]
        tracks = self.refs[0].shape[0] // self.crosses
        track = jnp.clip(self.track + shift, 0, tracks - 1)
        return self.refs[0][track * self.crosses + device, field, pl.ds(cell, 1), :]


def outer_kernel(ct, cc, crosses, nrefs, second, x_ref, v_ref, right_ref, *rest):
    track, c_index = lax.axis_index("track"), lax.axis_index("cross")
    vehicle = lax.axis_index("vehicle")
    vehicles, tracks = lax.axis_size("vehicle"), lax.axis_size("track")
    gathered = [Gathered(rest[:nrefs], crosses, track)]
    halos = [rest[nrefs]]
    rest = rest[nrefs + 1 :]
    if second:
        gathered.append(Gathered(rest[:1], crosses, track))
        halos.append(rest[1])
        rest = rest[2:]
    out_ref, state_ref, left_ref, sum_ref = rest
    wide = cc + 2
    has_low = c_index > 0
    has_high = c_index < crosses - 1
    put_own(state_ref, x_ref, v_ref, ct, cc)

    def place(slot, rr, p, load, ok):
        for axis in range(3):
            x, v = load(axis, 6, 0), load(axis + 3, 6, 0)
            if second:
                x, v = advanced(x, v, load(axis, 3, 1), axis)
            if axis == 0:
                x = x + (rr - (ct + 1) / 2)
                x = jnp.where(ok, x, far)
            if axis == 1:
                x = jnp.where(ok, x + (p - (cc + 1) / 2), 0.0)
            state_ref[pl.ds(slot * 8 + axis, 1), :] = x
            state_ref[pl.ds(slot * 8 + 3 + axis, 1), :] = jnp.where(ok, v, 0.0)

    def from_all(shift, row, p):
        step = -1 if p == 0 else (1 if p == cc + 1 else 0)
        device = jnp.clip(c_index + step, 0, crosses - 1)
        cell = row * cc + (p - 1) % cc
        return lambda f, n, k: gathered[k].line(shift, device, f, cell)

    def from_halo(p):
        return lambda f, n, k: halos[k][pl.ds(p * n + f, 1), :]

    for rr, shift, row in ((0, -1, ct - 1), (ct + 1, 1, 0)):
        if shift < 0:
            inside, exists = track > 0, (track > 0) | (vehicle > 0)
        else:
            inside = track < tracks - 1
            exists = inside | (vehicle < vehicles - 1)
        for p in range(wide):
            a, b = from_all(shift, row, p), from_halo(p)

            def load(f, n, k, a=a, b=b):
                return jnp.where(inside, a(f, n, k), b(f, n, k))

            ok = exists
            if p == 0:
                ok = jnp.logical_and(ok, has_low)
            if p == cc + 1:
                ok = jnp.logical_and(ok, has_high)
            place(rr * wide + p, rr, p, load, ok)
    for r in range(ct):
        place((r + 1) * wide, r + 1, 0, from_all(0, r, 0), has_low)
        place((r + 1) * wide + cc + 1, r + 1, cc + 1, from_all(0, r, cc + 1), has_high)
    ring = [rr * wide + p for rr in (0, ct + 1) for p in range(wide)]
    ring += [(r + 1) * wide + p for r in range(ct) for p in (0, cc + 1)]
    build_left(state_ref, left_ref, sum_ref, ring)

    jobs = []
    for c in range(cc):
        for r in range(ct):
            near = range(max(r - 1, 0), min(r + 2, ct))
            others = [(q + 1) * wide for q in near] if c == 0 else []
            others += [(q + 1) * wide + cc + 1 for q in near] if c == cc - 1 else []
            others += [c + d for d in range(3)] if r == 0 else []
            others += [(ct + 1) * wide + c + d for d in range(3)] if r == ct - 1 else []
            if others:
                jobs.append((r * cc + c, others))
    if ct > 2:
        out_ref[...] = jnp.zeros_like(out_ref)
    for (index, _), sums in zip(jobs, pushes(left_ref, sum_ref, right_ref, jobs)):
        start = ((index // cc + 1) * wide + index % cc + 1) * 8
        store_rows(out_ref, moment(state_ref[pl.ds(start, 8), :], sums), index, False)


def put_ring(state_ref, slot, across, along, load, second, ok):
    for axis in range(3):
        x, v = load(axis, 6, 0), load(axis + 3, 6, 0)
        if second:
            x, v = advanced(x, v, load(axis, 3, 1), axis)
        if axis == 0:
            x = jnp.where(ok, x + across, far)
        if axis == 1:
            x = jnp.where(ok, x + along, 0.0)
        state_ref[pl.ds(slot * 8 + axis, 1), :] = x
        state_ref[pl.ds(slot * 8 + 3 + axis, 1), :] = jnp.where(ok, v, 0.0)


def row_jobs(ct, cc, own_row):
    jobs = [(own_row * cc + c, [c + d for d in range(3)]) for c in range(cc)]
    starts = [((own_row + 1) * (cc + 2) + c + 1) * 8 for c in range(cc)]
    return jobs, [pl.multiple_of(start, 8) for start in starts]


def near_kernel(ct, cc, crosses, second, x_ref, v_ref, right_ref, *rest):
    track, c_index = lax.axis_index("track"), lax.axis_index("cross")
    gathered = [Gathered(rest[:2], crosses, track)]
    rest = rest[2:]
    if second:
        gathered.append(Gathered(rest[:1], crosses, track))
        rest = rest[1:]
    out_ref, state_ref, left_ref, sum_ref, own_ref = rest
    wide = cc + 2
    put_own(own_ref, x_ref, v_ref, ct, cc)
    has_low, has_high = c_index > 0, c_index < crosses - 1
    middle, centre = (ct + 1) / 2, (cc + 1) / 2
    first = track == 0
    shift = jnp.where(first, 1, -1)
    across = jnp.where(first, ct + 1 - middle, -middle)
    row = jnp.where(first, 0, ct - 1)

    def from_all(shift, row, p):
        step = -1 if p == 0 else (1 if p == cc + 1 else 0)
        device = jnp.clip(c_index + step, 0, crosses - 1)
        cell = row * cc + (p - 1) % cc
        return lambda f, n, k: gathered[k].line(shift, device, f, cell)

    for p in range(wide):
        ok = has_low if p == 0 else (has_high if p == cc + 1 else first | (track > 0))
        put_ring(state_ref, p, across, p - centre, from_all(shift, row, p), second, ok)
    sides = {}
    for r in range(ct):
        for p, ok in ((0, has_low), (cc + 1, has_high)):
            sides[r, p] = wide + len(sides)
            load = from_all(0, r, p)
            put_ring(state_ref, sides[r, p], r + 1 - middle, p - centre, load, second, ok)
    build_left(state_ref, left_ref, sum_ref, range(wide + len(sides)))
    jobs, starts = row_jobs(ct, cc, jnp.where(first, ct - 1, 0))
    for r in range(ct):
        near = range(max(r - 1, 0), min(r + 2, ct))
        for c, p in ((0, 0), (cc - 1, cc + 1)):
            jobs.append((r * cc + c, [sides[q, p] for q in near]))
            starts.append(((r + 1) * wide + c + 1) * 8)
    out_ref[...] = jnp.zeros_like(out_ref)
    for (index, _), start, sums in zip(jobs, starts, pushes(left_ref, sum_ref, right_ref, jobs)):
        store_rows(out_ref, moment(own_ref[pl.ds(start, 8), :], sums), index, True)


def far_kernel(ct, cc, crosses, second, x_ref, v_ref, right_ref, near_ref, *rest):
    track, c_index = lax.axis_index("track"), lax.axis_index("cross")
    vehicle, vehicles = lax.axis_index("vehicle"), lax.axis_size("vehicle")
    halos, rest = (rest[:2], rest[2:]) if second else (rest[:1], rest[1:])
    out_ref, state_ref, left_ref, sum_ref, own_ref = rest
    wide = cc + 2
    put_own(own_ref, x_ref, v_ref, ct, cc)
    middle, centre = (ct + 1) / 2, (cc + 1) / 2
    first = track == 0
    across = jnp.where(first, -middle, ct + 1 - middle)
    exists = jnp.where(first, vehicle, vehicles - 1 - vehicle) > 0
    for p in range(wide):
        ok = exists
        if p == 0:
            ok = ok & (c_index > 0)
        if p == cc + 1:
            ok = ok & (c_index < crosses - 1)

        def load(f, n, k, p=p):
            return halos[k][pl.ds(p * n + f, 1), :]

        put_ring(state_ref, p, across, p - centre, load, second, ok)
    build_left(state_ref, left_ref, sum_ref, range(wide))
    jobs, starts = row_jobs(ct, cc, jnp.where(first, 0, ct - 1))
    out_ref[...] = near_ref[...]
    for (index, _), start, sums in zip(jobs, starts, pushes(left_ref, sum_ref, right_ref, jobs)):
        store_rows(out_ref, moment(own_ref[pl.ds(start, 8), :], sums), index, True)


def face_kernel(
    second, ct, cc, crosses, nrefs, route_from, cell_from, offset_ref, velocity_ref, *rest
):
    all_refs, rest = rest[:nrefs], rest[nrefs:]
    if second:
        force_ref, before_ref, *rest = rest
    out_ref, react_ref, halo_ref, state_ref, face_ref, part_ref, route_ref, cell_ref, sems = rest
    copies = [
        pltpu.make_async_copy(route_from, route_ref, sems.at[0]),
        pltpu.make_async_copy(cell_from, cell_ref, sems.at[1]),
    ]
    for copy in copies:
        copy.start()
    devices, _, cells, _ = all_refs[0].shape
    count = offset_ref.shape[1]
    track = lax.axis_index("track")
    pack(ct, cc, crosses, track, [force_ref] if second else all_refs, halo_ref)
    starts = [jnp.bitwise_xor(k, track) * devices if nrefs == 2 else 0 for k in range(nrefs)]
    for k in range(nrefs):

        def spread(device, carry, k=k):
            base = pl.multiple_of((k * devices + device) * cells * 8, 8)
            for axis in range(3):
                x, v = all_refs[k][device, axis], all_refs[k][device, axis + 3]
                if second:
                    x, v = advanced(x, v, force_ref[starts[k] + device, axis], axis)
                state_ref[pl.ds(base + axis, cells, stride=8), :] = x
                state_ref[pl.ds(base + 3 + axis, cells, stride=8), :] = v
                part_ref[k * devices + device, axis] = jnp.zeros_like(x)
            return carry

        lax.fori_loop(0, devices, spread, 0, unroll=min(devices, 4))
    for axis in range(3):
        y, w = offset_ref[axis], velocity_ref[axis]
        if second:
            y = y + time_step * w
        face_ref[pl.ds(axis, count, stride=8), :] = y
        face_ref[pl.ds(3 + axis, count, stride=8), :] = w
    for copy in copies:
        copy.wait()

    def block_of(f):
        target = route_ref[f]
        where, across = lax.div(target, crosses), lax.rem(target, crosses)
        if nrefs == 2:
            where = jnp.bitwise_xor(where, track)
        return where * crosses + across, cell_ref[f]

    group = next(n for n in (faces_at_once, 16, 4, 2, 1) if count % n == 0)

    def several(g, carry):
        blocks, states, rights, back_sums, products, done = {}, {}, {}, {}, {}, {}
        faces, lefts, sums = {}, {}, {}
        for n in range(group + early + ahead + late):
            k = n
            if k < group:
                blocks[k] = block_of(g * group + k)
                place = (blocks[k][0] * cells + blocks[k][1]) * 8
                states[k] = state_ref[pl.ds(pl.multiple_of(place, 8), 8), :]
                pieces, row = features(states[k], soften * soften)
                rights[k], back_sums[k] = right_side(pieces, row), sum_side(pieces)
                faces[k] = face_ref[pl.ds(pl.multiple_of((g * group + k) * 8, 8), 8), :]
                pieces, _ = features(faces[k], 0.0)
                lefts[k], sums[k] = left_side(pieces, row), sum_side(pieces)
            k = n - early
            if 0 <= k < group:
                products[k] = dot(lefts.pop(k), rights.pop(k))
            k = n - early - ahead
            if 0 <= k < group:
                high, low = pair_weights(products.pop(k), radius + face_radius)
                done[k] = (
                    dot(sums.pop(k), jnp.concatenate([high, low], axis=0)),
                    dot(
                        back_sums.pop(k), jnp.concatenate([high, low], axis=1), ((1,), (1,))
                    ),
                )
            k = n - early - ahead - late
            if 0 <= k < group:
                f = g * group + k
                onto, back = done.pop(k)
                onto, back = moment(states.pop(k), onto), moment(faces.pop(k), back)
                device, cell = blocks[k]
                for axis in range(3):
                    line = time_step * damping * back[axis : axis + 1]
                    if second:
                        line = line + before_ref[axis, pl.ds(f, 1), :]
                    react_ref[axis, pl.ds(f, 1), :] = line
                    line = part_ref[device, axis, pl.ds(cell, 1), :]
                    line = line + damping * onto[axis : axis + 1]
                    part_ref[device, axis, pl.ds(cell, 1), :] = line
        return carry

    lax.fori_loop(0, count // group, several, 0)
    for k in range(nrefs):
        out_ref[pl.ds(starts[k], devices)] = part_ref[pl.ds(k * devices, devices)]


def pack(ct, cc, crosses, track, refs, out_ref):
    gathered = Gathered(refs, crosses, track)
    fields = refs[0].shape[1]
    c_index = lax.axis_index("cross")
    row = jnp.where(track < lax.axis_size("track") - 1, 0, ct - 1)
    for p in range(cc + 2):
        step = -1 if p == 0 else (1 if p == cc + 1 else 0)
        device = jnp.clip(c_index + step, 0, crosses - 1)
        cell = row * cc + (p - 1) % cc
        for f in range(fields):
            out_ref[pl.ds(p * fields + f, 1), :] = gathered.line(0, device, f, cell)


def first_kernel(
    count_from, x_from, v_from, own_ref, live_ref, spread_ref, count_ref, x_ref, v_ref, sems
):
    copies = [
        pltpu.make_async_copy(source, target, sems.at[k])
        for k, (source, target) in enumerate(
            ((count_from, count_ref), (x_from, x_ref), (v_from, v_ref))
        )
    ]
    for copy in copies:
        copy.start()
    for copy in copies:
        copy.wait()
    ct, cc = count_ref.shape
    shape = live_ref.shape
    row = lax.broadcasted_iota(jnp.int32, shape, 0)
    lane = lax.broadcasted_iota(jnp.int32, shape, 1)
    count = jnp.zeros(shape, jnp.int32)
    for cell in range(ct * cc):
        count = jnp.where(row == cell, count_ref[cell // cc, cell % cc], count)
    live = lane < count
    live_ref[...] = jnp.where(live, 1.0, 0.0)
    for axis in range(3):
        x, v = x_ref[axis], v_ref[axis]
        if axis == 0:
            x = jnp.where(live, x, far)
        own_ref[axis] = x
        for k in range(spread_ref.shape[0]):
            spread_ref[k, axis] = x
            spread_ref[k, axis + 3] = v


def update_kernel(second, live_ref, x_ref, v_ref, inner_ref, outer_ref, back_ref, *rest):
    if second:
        react_ref, *outs = rest
        outs[2][...] = react_ref[...]
    else:
        outs = rest
    live = live_ref[...] > 0.5
    for axis in range(3):
        force = jnp.where(live, inner_ref[axis] + outer_ref[axis], 0.0)
        for k in range(back_ref.shape[0]):
            force = force + back_ref[k, axis]
        x, v = advanced(x_ref[axis], v_ref[axis], force, axis)
        outs[0][axis] = x
        outs[1][axis] = v
        if not second:
            outs[2][axis] = jnp.where(live, x, far) if axis == 0 else x
            for k in range(back_ref.shape[0]):
                outs[3][k, axis] = force


def call(kernel, name, there, args, outs, scratch, flops, keep=True):
    specs = [pl.BlockSpec(memory_space=pltpu.HBM)] * len(there)
    specs += [pl.BlockSpec(memory_space=VMEM)] * len(args)
    there = [pltpu.with_memory_space_constraint(a, pltpu.HBM) for a in there]
    args = [pltpu.with_memory_space_constraint(a, VMEM_SPACE) for a in args]
    outs = [s if isinstance(s[0], tuple) else (s, f32) for s in outs]
    shapes = [VMEM(s, t) if keep else jax.ShapeDtypeStruct(s, t) for s, t in outs]
    return pl.pallas_call(
        kernel,
        name=name,
        out_shape=shapes,
        in_specs=specs,
        out_specs=[pl.BlockSpec(memory_space=VMEM)] * len(outs),
        scratch_shapes=scratch,
        compiler_params=pltpu.CompilerParams(vmem_limit_bytes=scratch_bytes),
        cost_estimate=pl.CostEstimate(flops=flops, transcendentals=0, bytes_accessed=0),
    )(*there, *args)


def body(
    particle_offset,
    particle_velocity,
    cell_count,
    face_offset,
    face_velocity,
    face_route,
    face_cell,
):
    _, ct, cc, slots = particle_offset.shape
    cells = ct * cc
    own_faces, _, faces = face_offset.shape
    vehicles, tracks, crosses = [lax.axis_size(a) for a in ("vehicle", "track", "cross")]
    pair = tracks == 2
    nrefs = 2 if pair else 1
    devices = tracks * crosses
    wide = cc + 2
    grid_slots = (ct + 2) * wide
    ring_slots = [
        VMEM((grid_slots * 8, slots), f32),
        VMEM((grid_slots, slots, 80), bf16),
        VMEM((grid_slots, 32, 2 * slots), bf16),
    ]
    right = ((cells, 80, 2 * slots), bf16)
    block = (3, cells, slots)
    swap = [(0, 1), (1, 0)]
    travel = []
    for e in range(vehicles - 1):
        last, following = e * tracks + tracks - 1, (e + 1) * tracks
        travel += [(last, following), (following, last)]

    def exchange(a, axes):
        return lax.all_to_all(a, axes, split_axis=0, concat_axis=0, tiled=True)

    def gather_track(a):
        if pair:
            return [a, lax.ppermute(a, "track", swap)]
        return [lax.all_gather(a, "track", axis=0, tiled=True)]

    x = particle_offset.reshape(block)
    v = particle_velocity.reshape(block)
    offset_rows = jnp.transpose(face_offset, (1, 0, 2))
    velocity_rows = jnp.transpose(face_velocity, (1, 0, 2))
    own, live, spread = call(
        first_kernel,
        "first",
        [cell_count, x, v],
        [],
        [block, (cells, slots), (crosses, 6, cells, slots)],
        [
            SMEM((ct, cc), jnp.int32),
            VMEM(block, f32),
            VMEM(block, f32),
            pltpu.SemaphoreType.DMA((3,)),
        ],
        10**6,
    )
    reaction = everyone = beyond = None
    for substep in range(2):
        second = substep == 1
        mine = exchange(spread, ("track", "cross") if second else "cross")
        inner, rights = call(
            functools.partial(inner_kernel, ct, cc),
            "inner",
            [],
            [own, v],
            [block, right],
            ring_slots,
            10**9,
        )
        mine, inner = lax.optimization_barrier((mine, inner))
        if second:
            extra, before = [mine], [reaction]
        else:
            everyone, extra, before = gather_track(mine), [], []
        part, reaction, packed = call(
            functools.partial(face_kernel, second, ct, cc, crosses, nrefs),
            "faces",
            [face_route.reshape(own_faces), face_cell],
            [offset_rows, velocity_rows] + everyone + extra + before,
            [
                (devices, 3, cells, slots),
                (3, own_faces, faces),
                (wide * (3 if second else 6), slots),
            ],
            [
                VMEM((devices * cells * 8, slots), f32),
                VMEM((own_faces * 8, faces), f32),
                VMEM((devices, 3, cells, slots), f32),
                SMEM((own_faces,), jnp.int32),
                SMEM((own_faces,), jnp.int32),
                pltpu.SemaphoreType.DMA((2,)),
            ],
            4 * 10**9,
        )
        across = lax.ppermute(packed, ("vehicle", "track"), travel)
        if second:
            halo_extra = [across]
        else:
            beyond, halo_extra = across, []
        if pair:
            near = call(
                functools.partial(near_kernel, ct, cc, crosses, second),
                "near",
                [],
                [own, v, rights] + everyone + extra,
                [block],
                ring_slots + ring_slots[:1],
                10**9,
            )[0]
            near, halo_now = lax.optimization_barrier((near, across))
            if second:
                halo_extra = [halo_now]
            else:
                beyond = halo_now
            outer = call(
                functools.partial(far_kernel, ct, cc, crosses, second),
                "far",
                [],
                [own, v, rights, near, beyond] + halo_extra,
                [block],
                ring_slots + ring_slots[:1],
                10**9,
            )[0]
        else:
            outer = call(
                functools.partial(outer_kernel, ct, cc, crosses, nrefs, second),
                "outer",
                [],
                [own, v, rights] + everyone + [beyond] + extra + halo_extra,
                [block],
                ring_slots,
                10**9,
            )[0]
        returned, outer = lax.optimization_barrier(
            (exchange(part, ("track", "cross")), outer)
        )
        new = call(
            functools.partial(update_kernel, second),
            "update",
            [],
            [live, x, v, inner, outer, returned] + ([reaction] if second else []),
            [block, block]
            + ([(3, own_faces, faces)] if second else [block, (devices, 3, cells, slots)]),
            [],
            10**6,
            not second,
        )
        x, v = new[:2]
        if second:
            reaction = new[2]
        else:
            own, spread = new[2:]
    shape = particle_offset.shape
    return (x.reshape(shape), v.reshape(shape), jnp.transpose(reaction, (1, 0, 2)))


def solution(mesh):
    in_specs = (
        P(None, ("vehicle", "track"), "cross", None),
        P(None, ("vehicle", "track"), "cross", None),
        P(("vehicle", "track"), "cross"),
        P(("vehicle", "track", "cross"), None, None),
        P(("vehicle", "track", "cross"), None, None),
        P(("vehicle", "track", "cross"), None),
        P(("vehicle", "track", "cross")),
    )
    out_specs = (
        P(None, ("vehicle", "track"), "cross", None),
        P(None, ("vehicle", "track"), "cross", None),
        P(("vehicle", "track", "cross"), None, None),
    )
    return jax.shard_map(body, mesh=mesh, in_specs=in_specs, out_specs=out_specs, check_vma=False)
```
